256 devices in a mesh: seq: 32 (over z, y_hi, core), batch: 8 (over x, y_lo).
Axes of the slice: x: 4, y: 4 (y_hi: 2, y_lo: 2; y = y_hi * 2 + y_lo), z: 8, core: 2. Of those that a mesh axis runs over, the one named last changes fastest.
Arguments:
- queries: bfloat16 [32768, 1792], P(('batch', 'seq')), parts along dimension 0, may hold values from -128 to 128
- keys: bfloat16 [32768, 256], P(('batch', 'seq')), parts along dimension 0, may hold values from -4 to 4
- values: bfloat16 [32768, 256], P(('batch', 'seq')), parts along dimension 0, may hold values from -4 to 4
- out_grad: bfloat16 [32768, 1792], P(('batch', 'seq')), parts along dimension 0, may hold values from -24 to 24
- row_delta: float32 [32768, 14], P(('batch', 'seq')), parts along dimension 0, may hold values from -6 to 6
- layer_input: bfloat16 [32768, 3584], P(('batch', 'seq')), parts along dimension 0, may hold values from -6 to 6
- norm_gain: float32 [3584], replicated, may hold values from 0.25 to 1.75
- qkv_weight: bfloat16 [3584, 2304], P('seq'), may hold values from -0.5 to 0.5
- block_order: int32 [512], P('batch'), parts along dimension 0, may hold values from 0 to 63, as said below
- block_mask: int32 [512, 64], P('batch'), parts along dimension 0, may hold values from 0 to 1, as said below
- frame_owner: int32 [256], P('batch'), parts along dimension 0, may hold values from 0 to 31, as said below
- vision_features: bfloat16 [256, 128, 1152], P(('batch', 'seq')), parts along dimension 0, may hold values from -6 to 6
- post_gain: float32 [1152], replicated, may hold values from 0.25 to 1.75
- projector: bfloat16 [1152, 3584], replicated, may hold values from -0.1875 to 0.1875
Outputs:
- token_grad: bfloat16 [32768, 3584], P(('batch', 'seq')), parts along dimension 0
- encoder_grad: bfloat16 [256, 128, 1152], P(('batch', 'seq')), parts along dimension 0
The draws below stay inside these ranges and needn't reach their ends.
There are 8 independent parts, one for each index of `batch`. The reference program is written for one: setup_inputs(seed, part) draws one part's arguments, and reference() takes and returns one part's arrays. A program takes and returns all parts, laid end to end along the dimension named above; an argument that names none is the same for every part. Nothing has to cross between parts.
Inputs may be any that keep to these rules, and one draw needn't show every extreme that they name: `block_order`: entries 2i and 2i + 1 are the blocks of device i of seq; all entries together are a permutation; each device's two blocks sum to 63; for every frame f, blocks 2f and 2f + 1 lie on devices 2j and 2j + 1 for some j. `block_mask`: 1 on the diagonal, 0 above it. `frame_owner`: every device of seq owns exactly one frame, and the owner of frame f holds block 2f or block 2f + 1.
All inputs are finite; a program needn't handle non-finite values.
Results may differ from the reference program's by a relative error of at most 0.012.
Values may be sent and summed in bfloat16 or wider, within the bound.
A program may use at most 128 MiB of HBM per device.

```python
import jax
import jax.numpy as jnp
from jax import lax

D = 3584
HQ = 14
KVH = 2
HD = 128
C_ENC = 1152
TOK_DEV = 128
QKV = 2304
SEQ_LEN = 4096
FRAMES = 32
N_SEQ = 32


def frame_layout(key):
    count = N_SEQ
    groups = count // 2
    slot = jax.random.permutation(jax.random.fold_in(key, 11), groups).astype(jnp.int32)
    flip = jax.random.randint(jax.random.fold_in(key, 12), (groups,), 0, 2).astype(jnp.int32)
    order_first = jax.random.randint(jax.random.fold_in(key, 13), (groups,), 0, 2).astype(jnp.int32)
    order_second = jax.random.randint(jax.random.fold_in(key, 14), (groups,), 0, 2).astype(jnp.int32)
    owner_bit = jax.random.randint(jax.random.fold_in(key, 15), (groups,), 0, 2).astype(jnp.int32)
    group_ids = jnp.arange(groups, dtype=jnp.int32)
    device_first = (2 * slot + flip).astype(jnp.int32)
    device_second = (2 * slot + 1 - flip).astype(jnp.int32)
    first_lead = jnp.where(order_first == 1, 2 * count - 1 - 2 * group_ids, 2 * group_ids).astype(jnp.int32)
    second_lead = jnp.where(order_second == 1, 2 * count - 2 - 2 * group_ids, 2 * group_ids + 1).astype(jnp.int32)
    order = jnp.zeros((2 * count,), jnp.int32)
    order = order.at[2 * device_first].set(first_lead).at[2 * device_first + 1].set(2 * count - 1 - first_lead)
    order = order.at[2 * device_second].set(second_lead).at[2 * device_second + 1].set(2 * count - 1 - second_lead)
    owner = jnp.zeros((count,), jnp.int32)
    owner = owner.at[group_ids].set(jnp.where(owner_bit == 1, device_second, device_first))
    owner = owner.at[count - 1 - group_ids].set(jnp.where(owner_bit == 1, device_first, device_second))
    return (order.astype(jnp.int32), owner.astype(jnp.int32))


def draw_block_order(key, part):
    return frame_layout(key)[0]


def draw_frame_owner(key, part):
    return frame_layout(key)[1]


def draw_block_mask(key, part):
    count_blocks = 2 * N_SEQ
    random_bits = jax.random.randint(jax.random.fold_in(key, 21), (count_blocks, count_blocks), 0, 2).astype(jnp.int32)
    row_index = jnp.arange(count_blocks, dtype=jnp.int32)[:, None]
    column_index = jnp.arange(count_blocks, dtype=jnp.int32)[None, :]
    return jnp.where(row_index > column_index, random_bits, jnp.where(row_index == column_index, 1, 0)).astype(jnp.int32)


def attention_inputs(key):
    total_rows = TOK_DEV * N_SEQ
    half_len = TOK_DEV // 2
    group_size = HQ // KVH
    count_blocks = 2 * N_SEQ
    ranking = jnp.stack([jax.random.permutation(jax.random.fold_in(key, 40 + head), HD) for head in range(KVH)]).astype(jnp.int32)
    dim_scale = jnp.where(ranking < HD // 2, 1.5, 0.5).astype(jnp.float32)
    block_scale = jnp.exp(jax.random.uniform(jax.random.fold_in(key, 41), (count_blocks, 1, KVH, HD), jnp.float32, jnp.log(0.7), jnp.log(1.4)))
    key_scale = dim_scale[None, None, :, :] * block_scale
    limit = 4.0 / key_scale
    key_base = jax.random.truncated_normal(jax.random.fold_in(key, 31), -limit, limit, (count_blocks, half_len, KVH, HD), jnp.float32)
    keys_drawn = (key_base * key_scale).reshape(total_rows, KVH, HD)
    query_base = jax.random.truncated_normal(jax.random.fold_in(key, 32), -4.0, 4.0, (total_rows, KVH, group_size, HD), jnp.float32)
    queries_drawn = query_base * dim_scale[None, :, None, :]
    return (queries_drawn.reshape(total_rows, HQ * HD), keys_drawn.reshape(total_rows, KVH * HD))


def draw_queries(key, part):
    return attention_inputs(key)[0].astype(jnp.bfloat16)


def draw_keys(key, part):
    return attention_inputs(key)[1].astype(jnp.bfloat16)


def level_of(key, extent, cuts, smallest, largest):
    factor_of, own = 1.0, jax.random.fold_in(key, 6)
    for dim, shards_of in cuts:
        heights = jnp.exp(jax.random.uniform(jax.random.fold_in(own, dim), (shards_of,), jnp.float32, smallest / len(cuts), largest / len(cuts)))
        factor_of = factor_of * jnp.repeat(heights, extent[dim] // shards_of).reshape([-1 if axis == dim else 1 for axis in range(len(extent))])
    return factor_of


def gaussian(key, dims, scale, most, cuts=(), held_as=jnp.bfloat16):
    values = jax.random.normal(key, dims, jnp.float32) * scale
    if len(cuts) > 0:
        values = level_of(key, dims, cuts, -0.22, 0.18) * values
    return jnp.clip(values, min=-most, max=most).astype(held_as)


def setup_inputs(seed: int = 0, part: int = 0) -> dict:
    key_of = jax.random.split(jax.random.key(seed), 15)
    part_splits = jax.random.split(jax.random.fold_in(key_of[14], part), 15)
    return {
        "queries": draw_queries(jax.random.fold_in(jax.random.fold_in(key_of[14], part), 71), part),
        "keys": draw_keys(jax.random.fold_in(jax.random.fold_in(key_of[14], part), 71), part),
        "values": gaussian(part_splits[2], (SEQ_LEN, KVH * HD), 1.0, 4.0, ((0, 32),)),
        "out_grad": gaussian(part_splits[3], (SEQ_LEN, HQ * HD), 4.0, 24.0, ((0, 32),)),
        "row_delta": gaussian(part_splits[4], (SEQ_LEN, HQ), 1.0, 6.0, ((0, 32),), jnp.float32),
        "layer_input": gaussian(part_splits[5], (SEQ_LEN, D), 1.0, 6.0, ((0, 32),)),
        "norm_gain": jnp.clip(1.0 + 0.15 * jax.random.normal(key_of[6], (D,), jnp.float32), 0.25, 1.75),
        "qkv_weight": gaussian(key_of[7], (D, QKV), HD ** -0.5, 0.5, ((0, 32),)),
        "block_order": draw_block_order(jax.random.fold_in(jax.random.fold_in(key_of[14], part), 71), part),
        "block_mask": draw_block_mask(jax.random.fold_in(jax.random.fold_in(key_of[14], part), 71), part),
        "frame_owner": draw_frame_owner(jax.random.fold_in(jax.random.fold_in(key_of[14], part), 71), part),
        "vision_features": gaussian(part_splits[11], (FRAMES, TOK_DEV, C_ENC), 1.0, 6.0, ((0, 32),)),
        "post_gain": jnp.clip(1.0 + 0.15 * jax.random.normal(key_of[12], (C_ENC,), jnp.float32), 0.25, 1.75),
        "projector": gaussian(key_of[13], (C_ENC, D), C_ENC ** -0.5, 0.1875),
    }


EPSILON = 1e-06
NEGATIVE = -1e+30

def reference(queries, keys, values, out_grad, row_delta, layer_input, norm_gain, qkv_weight, block_order, block_mask, frame_owner, vision_features, post_gain, projector):
    half_len = TOK_DEV // 2
    total_rows = TOK_DEV * N_SEQ
    group_size = HQ // KVH
    scaling = HD ** (-0.5)
    row_ids = jnp.arange(total_rows, dtype=jnp.int32)
    position = (block_order[row_ids // half_len] * half_len + row_ids % half_len).astype(jnp.int32)
    blocks = (position // half_len).astype(jnp.int32)
    query_heads = queries.reshape(total_rows, HQ, HD)
    grad_heads = out_grad.reshape(total_rows, HQ, HD)
    key_heads = keys.reshape(total_rows, KVH, HD)
    value_heads = values.reshape(total_rows, KVH, HD)

    def one_head(head_index):
        kv_index = (head_index // group_size).astype(jnp.int32)
        query_rows = lax.dynamic_index_in_dim(query_heads, head_index, 1, keepdims=False)
        grad_rows = lax.dynamic_index_in_dim(grad_heads, head_index, 1, keepdims=False)
        key_rows = lax.dynamic_index_in_dim(key_heads, kv_index, 1, keepdims=False)
        value_rows = lax.dynamic_index_in_dim(value_heads, kv_index, 1, keepdims=False)
        delta_rows = lax.dynamic_index_in_dim(row_delta, head_index, 1, keepdims=False)

        def per_block(running, block_start):
            key_acc, value_acc = running
            query_block = lax.dynamic_slice_in_dim(query_rows, block_start, TOK_DEV, 0)
            grad_block = lax.dynamic_slice_in_dim(grad_rows, block_start, TOK_DEV, 0)
            delta_block = lax.dynamic_slice_in_dim(delta_rows, block_start, TOK_DEV, 0)
            pos_block = lax.dynamic_slice_in_dim(position, block_start, TOK_DEV, 0)
            block_ids = lax.dynamic_slice_in_dim(blocks, block_start, TOK_DEV, 0)
            allowed = (block_mask[block_ids][:, blocks] == 1) & (position[None, :] <= pos_block[:, None])
            score = jnp.dot(query_block, key_rows.T, preferred_element_type=jnp.float32) * scaling
            top_score = lax.optimization_barrier(jnp.max(jnp.where(allowed, score, NEGATIVE), axis=1))
            total_exp = lax.optimization_barrier(jnp.sum(jnp.where(allowed, jnp.exp(score - top_score[:, None]), 0.0), axis=1))
            lse = top_score + jnp.log(total_exp)
            prob = jnp.where(allowed, jnp.exp(score - lse[:, None]), 0.0)
            prob_low = prob.astype(jnp.bfloat16)
            value_acc = value_acc + jnp.dot(prob_low.T, grad_block, preferred_element_type=jnp.float32)
            prob_grad = jnp.dot(grad_block, value_rows.T, preferred_element_type=jnp.float32)
            score_grad = (prob * (prob_grad - delta_block[:, None])).astype(jnp.bfloat16)
            query_out = jnp.dot(score_grad, key_rows, preferred_element_type=jnp.float32) * scaling
            key_acc = key_acc + jnp.dot(score_grad.T, query_block, preferred_element_type=jnp.float32)
            return ((key_acc, value_acc), query_out)
        starting = (jnp.zeros((total_rows, HD), jnp.float32), jnp.zeros((total_rows, HD), jnp.float32))
        starts = (jnp.arange(N_SEQ, dtype=jnp.int32) * TOK_DEV).astype(jnp.int32)
        finals, query_parts = lax.scan(per_block, starting, starts)
        return (query_parts.reshape(total_rows, HD), finals[0] * scaling, finals[1])
    query_all, key_all, value_all = lax.map(one_head, jnp.arange(HQ, dtype=jnp.int32))
    query_grad = jnp.transpose(query_all, (1, 0, 2)).reshape(total_rows, HQ * HD)
    key_grad = jnp.transpose(lax.optimization_barrier(jnp.sum(key_all.reshape(KVH, group_size, total_rows, HD), axis=1)), (1, 0, 2)).reshape(total_rows, KVH * HD)
    value_grad = jnp.transpose(lax.optimization_barrier(jnp.sum(value_all.reshape(KVH, group_size, total_rows, HD), axis=1)), (1, 0, 2)).reshape(total_rows, KVH * HD)
    head_grads = jnp.concatenate([query_grad, key_grad, value_grad], axis=1).astype(jnp.bfloat16)
    norm_grad = jnp.dot(head_grads, qkv_weight.T, preferred_element_type=jnp.float32).astype(jnp.bfloat16)
    inputs = layer_input.astype(jnp.float32)
    inverse = lax.rsqrt(lax.optimization_barrier(jnp.mean(inputs * inputs, axis=1, keepdims=True)) + EPSILON)
    scaled = norm_grad.astype(jnp.float32) * norm_gain
    token_grad = (inverse * scaled - inputs * inverse ** 3 * lax.optimization_barrier(jnp.mean(scaled * inputs, axis=1, keepdims=True))).astype(jnp.bfloat16)
    row_of_position = jnp.zeros((total_rows,), jnp.int32).at[position].set(row_ids)
    device_ids = jnp.arange(N_SEQ, dtype=jnp.int32)
    frame_of_device = jnp.zeros((N_SEQ,), jnp.int32).at[frame_owner].set(device_ids)
    spatial = jnp.arange(TOK_DEV, dtype=jnp.int32)
    frame_rows = row_of_position[(frame_of_device[:, None] * TOK_DEV + spatial[None, :]).astype(jnp.int32)]
    frame_grad = token_grad[frame_rows]
    post_grad = jnp.dot(frame_grad.reshape(N_SEQ * TOK_DEV, D), projector.T, preferred_element_type=jnp.float32).reshape(N_SEQ, TOK_DEV, C_ENC)
    features = vision_features.astype(jnp.float32)
    centered = features - lax.optimization_barrier(jnp.mean(features, axis=2, keepdims=True))
    deviation = lax.rsqrt(lax.optimization_barrier(jnp.mean(centered * centered, axis=2, keepdims=True)) + EPSILON)
    normed = centered * deviation
    weighted = post_grad * post_gain
    encoder_grad = (deviation * (weighted - lax.optimization_barrier(jnp.mean(weighted, axis=2, keepdims=True)) - normed * lax.optimization_barrier(jnp.mean(weighted * normed, axis=2, keepdims=True)))).astype(jnp.bfloat16)
    return (token_grad, encoder_grad)
```

```python
import jax
import jax.numpy as jnp
from jax import lax
from jax.experimental import pallas as pl
from jax.experimental.pallas import tpu as pltpu
from jax.sharding import PartitionSpec as P

HG = 7
HD = 128
GW = 896
CW = 1152
D = 3584
WR = 112
EPSILON = 1e-06
LOG2E = 1.4426950408889634
SCALE = 128 ** -0.5
TILE = 256
BF = jnp.bfloat16
F32 = jnp.float32
MESH = pl.DeviceIdType.MESH


class Place:
    def __init__(self):
        s = lax.axis_index("seq")
        b = lax.axis_index("batch")
        self.s = s
        self.c = s % 2
        self.h = (s // 2) % 2
        self.z = s // 4
        self.l = b % 2
        self.x = b // 2
        self.unit = (self.x + 2 * self.l) % 4

    def dev(self, dz=0, h=None, c=None, dx=0, l=None):
        z = (self.z + dz + 8) % 8
        x = (self.x + dx + 4) % 4
        h = self.h if h is None else h
        c = self.c if c is None else c
        l = self.l if l is None else l
        return {"seq": (z * 2 + h) * 2 + c, "batch": x * 2 + l}

    def chip(self, dz, h):
        return ((self.z + dz + 8) % 8) * 2 + h


class Links:
    def __init__(self, send, recv):
        self.send, self.recv, self.used = send, recv, 0

    def copy(self, src, dst, dev):
        i = self.used
        self.used += 1
        return pltpu.make_async_remote_copy(
            src_ref=src, dst_ref=dst, send_sem=self.send.at[i], recv_sem=self.recv.at[i],
            device_id=dev, device_id_type=MESH)


def greet(devs):
    barrier = pltpu.get_barrier_semaphore()
    for d in devs:
        pl.semaphore_signal(barrier, inc=1, device_id=d, device_id_type=MESH)
    pl.semaphore_wait(barrier, len(devs))


def weight_parts(half):
    return ((half * GW, GW, 0), (HG * 2 * HD + half * HD, HD, GW), (HG * 2 * HD + 2 * HD + half * HD, HD, GW + HD))


IN_LINKS = 96
LEVELS = 5


def gather_kernel(k_ref, v_ref, q_ref, do_ref, dl_ref, w_ref, kvg, q2, do2, dl2, wg, w2, away, wu, w0, send, recv, loc):
    p = Place()
    links = Links(send, recv)
    partner = p.dev(c=1 - p.c)
    across = [p.dev(h=1 - p.h, l=1 - p.l, c=0), p.dev(h=1 - p.h, l=1 - p.l, c=1)]
    ypeer = p.dev(h=1 - p.h)
    zs = {1: p.dev(dz=1), -1: p.dev(dz=-1)}
    fan = [p.dev(dx=1), p.dev(dx=-1), p.dev(l=1 - p.l)]
    mine, other = p.c, 1 - p.c
    col = lambda i, w: pl.ds(pl.multiple_of(i * w, 128), w)
    sent = []
    own = [pltpu.make_async_copy(k_ref.at[:, col(mine, HD)], kvg.at[p.s, 0], loc.at[0]),
           pltpu.make_async_copy(v_ref.at[:, col(mine, HD)], kvg.at[p.s, 1], loc.at[1])]
    pack = [pltpu.make_async_copy(k_ref.at[:, col(other, HD)], away.at[0], loc.at[2]),
            pltpu.make_async_copy(v_ref.at[:, col(other, HD)], away.at[1], loc.at[3])]
    rest = [pltpu.make_async_copy(q_ref.at[:, col(mine, GW)], q2.at[p.c], loc.at[4]),
            pltpu.make_async_copy(do_ref.at[:, col(mine, GW)], do2.at[p.c], loc.at[5]),
            pltpu.make_async_copy(dl_ref.at[mine], dl2.at[p.c], loc.at[6])]
    for cp in own + pack + rest:
        cp.start()
    greet([partner, ypeer] + across + [zs[1], zs[-1]] + fan)

    def begin(cp):
        cp.start()
        sent.append(cp)
        return cp

    swap = links.copy(away, kvg.at[p.s], partner)
    for cp in pack:
        cp.wait()
    begin(swap)
    for cp in own:
        cp.wait()
    kv = {}
    slot = lambda dz, e, q: 2 * p.chip(dz, p.h if e == 0 else 1 - p.h) + (p.c if q == 0 else 1 - p.c)

    def kv_send(step, e, q, dr):
        block = kvg.at[slot(-dr * (step - 1), e, q)]
        kv[step, e, q, dr] = begin(links.copy(block, block, zs[dr]))

    def y_send(q):
        block = kvg.at[slot(0, 0, q)]
        return begin(links.copy(block, block, ypeer))

    sy = {0: y_send(0)}
    for dr in (1, -1):
        kv_send(1, 0, 0, dr)

    lead = p.unit % 2 == p.c
    to_partner, to_self, to_across = [], [], []
    for i, (start, width, at) in enumerate(weight_parts(other)):
        to_partner.append(links.copy(w_ref.at[:, pl.ds(pl.multiple_of(start, 128), width)],
                                     w0.at[2 * p.h + p.c, :, pl.ds(at, width)], partner))
    for i, (start, width, at) in enumerate(weight_parts(mine)):
        to_self.append(pltpu.make_async_copy(w_ref.at[:, pl.ds(pl.multiple_of(start, 128), width)],
                                             w0.at[2 * p.h + p.c, :, pl.ds(at, width)], loc.at[7 + i]))
    for half in (0, 1):
        for i, (start, width, at) in enumerate(weight_parts(half)):
            n = links.used
            links.used += 1
            to_across.append((p.c, half, i, w_ref.at[:, pl.ds(start, width)], w0.at[2 * p.h + p.c, :, pl.ds(at, width)], n))
    first = IN_LINKS - 6
    to_across = [pltpu.make_async_remote_copy(
        src_ref=src, dst_ref=dst, send_sem=send.at[n], recv_sem=recv.at[first + 3 * d + i],
        device_id=across[half], device_id_type=MESH) for d, half, i, src, dst, n in to_across]
    from_across = [[pltpu.make_async_remote_copy(
        src_ref=w_ref.at[:, pl.ds(start, width)], dst_ref=w0.at[2 * (1 - p.h) + d, :, pl.ds(at, width)],
        send_sem=send.at[0], recv_sem=recv.at[first + 3 * d + i],
        device_id=across[0], device_id_type=MESH) for i, (start, width, at) in enumerate(weight_parts(0))] for d in (0, 1)]
    for cp in to_self:
        cp.start()
    for cp in to_partner:
        begin(cp)

    @pl.when(lead)
    def _():
        for cp in to_across:
            cp.start()

    swap.wait_recv()
    sy[1] = y_send(1)
    for dr in (1, -1):
        kv_send(1, 0, 1, dr)

    side = [links.copy(q_ref.at[:, col(other, GW)], q2.at[p.c], partner),
            links.copy(do_ref.at[:, col(other, GW)], do2.at[p.c], partner),
            links.copy(dl_ref.at[other], dl2.at[p.c], partner)]
    for cp in side:
        begin(cp)
    for q in (0, 1):
        sy[q].wait_recv()
        for dr in (1, -1):
            kv_send(1, 1, q, dr)

    wz, fans, keep = {}, {}, []

    def store(src, dst):
        cp = pltpu.make_async_copy(src, dst, loc.at[10 + len(keep)])
        cp.start()
        keep.append(cp)

    def w_send(step):
        for dr in (1, -1):
            src = w0.at[p.unit] if step == 1 else wu.at[2 - dr * (step - 1)]
            wz[step, dr] = begin(links.copy(src, wu.at[2 - dr * step], zs[dr]))

    def w_take(step):
        for dr in (1, -1):
            wz[step, dr].wait_recv()
        if step == 1:
            w_send(2)
            for dr in (1, -1):
                for n, dev in enumerate(fan):
                    fans[dr, n] = begin(links.copy(wu.at[2 - dr], wg.at[1 - dr, 1 + n], dev))
                store(wu.at[2 - dr], wg.at[1 - dr, 0])
        else:
            for dr in (1, -1):
                store(wu.at[2 - 2 * dr], w2.at[(1 - dr) // 2])

    def kv_step(step, e):
        for q in (0, 1):
            for dr in (1, -1):
                kv[step, e, q, dr].wait_recv()
                if step < 3 or (dr == 1) == (e == 0):
                    kv_send(step + 1, e, q, dr)

    for cp in to_self:
        cp.wait()
    for cp in to_partner:
        cp.wait_recv()

    for d in (0, 1):
        @pl.when(p.unit % 2 == d)
        def _():
            for cp in from_across[d]:
                cp.wait_recv()
    w_send(1)
    kv_step(1, 0)

    @pl.when(jnp.logical_not(lead))
    def _():
        for cp in to_across:
            cp.start()
    kv_step(1, 1)
    kv_step(2, 0)
    w_take(1)
    kv_step(2, 1)
    kv_step(3, 0)
    w_take(2)
    kv_step(3, 1)
    for d in (0, 1):
        @pl.when(p.unit % 2 != d)
        def _():
            for cp in from_across[d]:
                cp.wait_recv()
    for n, turn in enumerate((0, 3, 1, 2)):
        store(w0.at[(p.unit + turn) % 4], wg.at[1, n])
    for q in (0, 1):
        kv[4, 0, q, 1].wait_recv()
        kv[4, 1, q, -1].wait_recv()
    for cp in fans.values():
        cp.wait_recv()
    for cp in rest + keep:
        cp.wait()
    for cp in side:
        cp.wait_recv()
    for cp in sent:
        cp.wait_send()

    for cp in to_across:
        cp.wait_send()


def gather(keys, values, queries, out_grad, delta, weight):
    hbm = pl.BlockSpec(memory_space=pl.ANY)
    vmem = pl.BlockSpec(memory_space=pltpu.VMEM)
    return pl.pallas_call(
        gather_kernel,
        out_shape=(jax.ShapeDtypeStruct((32, 2, 128, HD), BF), jax.ShapeDtypeStruct((2, 128, GW), BF),
                   jax.ShapeDtypeStruct((2, 128, GW), BF), jax.ShapeDtypeStruct((2, 8, 128), F32),
                   jax.ShapeDtypeStruct((3, 4, WR, CW), BF), jax.ShapeDtypeStruct((2, WR, CW), BF)),
        in_specs=[hbm] * 6,
        out_specs=(vmem, vmem, vmem, vmem, hbm, hbm),
        scratch_shapes=[pltpu.VMEM((2, 128, HD), BF), pltpu.VMEM((LEVELS, WR, CW), BF), pltpu.VMEM((4, WR, CW), BF),
                        pltpu.SemaphoreType.DMA((IN_LINKS,)), pltpu.SemaphoreType.DMA((IN_LINKS,)),
                        pltpu.SemaphoreType.DMA((24,))],
        compiler_params=pltpu.CompilerParams(collective_id=0, has_side_effects=True),
        name="gather",
    )(keys, values, queries, out_grad, delta, weight)


def attn_kernel(order_ref, mask_ref, q_ref, do_ref, delta_ref, kv_ref, dq_ref, dkv_ref,
                inv_ref, live_ref, dks, dvs, qs, qt, dos, dot_, m_ref, l_ref, dl_ref, dqt):
    chip = lax.axis_index("seq") // 2

    def invert(i, _):
        inv_ref[order_ref[i]] = i
        return 0
    lax.fori_loop(0, 64, invert, 0, unroll=8)
    dks[...] = jnp.zeros_like(dks)
    dvs[...] = jnp.zeros_like(dvs)
    qs[HG * 64:, :] = jnp.zeros((64, HD), BF)
    dos[HG * 64:, :] = jnp.zeros((64, HD), BF)
    lane8 = lax.broadcasted_iota(jnp.int32, (1, 128), 1)
    ahead = lax.broadcasted_iota(jnp.int32, (64, 128), 0) - lax.broadcasted_iota(jnp.int32, (64, 128), 1) % 64

    def query_block(i, _):
        block = order_ref[4 * chip + i]
        dev, odd = i // 2, i % 2
        half = pl.multiple_of(odd * 64, 64)
        for src, st, tr in ((q_ref, qs, qt), (do_ref, dos, dot_)):
            for h in range(HG):
                st[h * 64:(h + 1) * 64, :] = src[dev, pl.ds(half, 64), h * HD:(h + 1) * HD]
            for r in range(4):
                tr[:, r * 128:(r + 1) * 128] = st[r * 128:(r + 1) * 128, :].T
        delta = delta_ref[dev]
        turned = pltpu.roll(delta, 64, 1)
        first = jnp.where(odd == 0, delta, turned)
        second = jnp.where(odd == 0, turned, delta)
        for r in range(4):
            dl_ref[r:r + 1, :] = jnp.where(lane8 < 64, first[2 * r:2 * r + 1], second[2 * r + 1:2 * r + 2])
        m_ref[...] = jnp.full_like(m_ref, -1e20)
        l_ref[...] = jnp.zeros_like(l_ref)
        dqt[...] = jnp.zeros_like(dqt)

        def collect(kb, n):
            live_ref[n] = inv_ref[kb]
            return n + jnp.where((mask_ref[block, kb] > 0) & (kb < block), 1, 0)
        count = lax.fori_loop(0, 64, collect, jnp.int32(0), unroll=8)
        for e in range(4):
            live_ref[count + e] = inv_ref[block]
        last = count // 4

        def places(t):
            out = []
            for e in range(4):
                k = live_ref[t * 4 + e]
                out.append((k // 2, pl.ds(pl.multiple_of((k % 2) * 64, 64), 64)))
            return out

        def bias_of(t):
            parts = []
            for e in range(4):
                index = t * 4 + e
                reach = jnp.where(index < count, 64, jnp.where(index == count, 0, -64))
                parts.append(jnp.where(ahead <= reach, 0.0, -1e30))
            return jnp.concatenate(parts, axis=0)

        def totals(t, masked):
            k = jnp.concatenate([kv_ref[d, 0, r, :] for d, r in places(t)], axis=0)
            s = jnp.dot(k, qt[...], preferred_element_type=F32)
            bias = bias_of(t) if masked else None
            for r in range(4):
                sh = s[:, r * 128:(r + 1) * 128] * (SCALE * LOG2E)
                if masked:
                    sh = sh + bias
                m_old = m_ref[r:r + 1, :]
                m_new = jnp.maximum(m_old, jnp.max(sh, axis=0, keepdims=True))
                p = jnp.exp2(sh - m_new)
                l_ref[r:r + 1, :] = l_ref[r:r + 1, :] * jnp.exp2(m_old - m_new) + jnp.sum(p, axis=0, keepdims=True)
                m_ref[r:r + 1, :] = m_new

        def totals_step(t, _):
            totals(t, False)
            return 0
        lax.fori_loop(0, last, totals_step, 0)
        totals(last, True)
        m_ref[0:4, :] = m_ref[0:4, :] + jnp.log2(l_ref[0:4, :])

        def grads(t, masked):
            at = places(t)
            k = jnp.concatenate([kv_ref[d, 0, r, :] for d, r in at], axis=0)
            v = jnp.concatenate([kv_ref[d, 1, r, :] for d, r in at], axis=0)
            s = jnp.dot(k, qt[...], preferred_element_type=F32)
            dp = jnp.dot(v, dot_[...], preferred_element_type=F32)
            bias = bias_of(t) if masked else None
            ps, dss = [], []
            for r in range(4):
                cols = slice(r * 128, (r + 1) * 128)
                sh = s[:, cols] * (SCALE * LOG2E) - m_ref[r:r + 1, :]
                if masked:
                    sh = sh + bias
                p = jnp.exp2(sh)
                ds = p * (dp[:, cols] - dl_ref[r:r + 1, :])
                ps.append(p.astype(BF))
                dss.append(ds.astype(BF))
            p = jnp.concatenate(ps, axis=1)
            ds = jnp.concatenate(dss, axis=1)
            dv = jnp.dot(p, dos[...], preferred_element_type=F32)
            dk = jnp.dot(ds, qs[...], preferred_element_type=F32)
            for e, (d, r) in enumerate(at):
                dvs[d, r, :] += dv[e * 64:(e + 1) * 64]
                dks[d, r, :] += dk[e * 64:(e + 1) * 64]
            dqt[...] += jnp.dot(k.T, ds, preferred_element_type=F32)

        def grads_step(t, _):
            grads(t, False)
            return 0
        lax.fori_loop(0, last, grads_step, 0)
        grads(last, True)
        for r in range(4):
            out = (dqt[:, r * 128:(r + 1) * 128].T * SCALE).astype(BF)
            for e in range(2):
                if 2 * r + e < HG:
                    dq_ref[dev, pl.ds(half, 64), (2 * r + e) * HD:(2 * r + e + 1) * HD] = out[e * 64:(e + 1) * 64]
        return 0
    lax.fori_loop(0, 4, query_block, 0)

    def write_out(d, _):
        dkv_ref[d, 0] = (dks[d] * SCALE).astype(BF)
        dkv_ref[d, 1] = dvs[d].astype(BF)
        return 0
    lax.fori_loop(0, 32, write_out, 0)


def attn(order, mask, q2, do2, delta2, kvg):
    smem = pl.BlockSpec(memory_space=pltpu.SMEM)
    vmem = pl.BlockSpec(memory_space=pltpu.VMEM)
    return pl.pallas_call(
        attn_kernel,
        out_shape=(jax.ShapeDtypeStruct((2, 128, GW), BF), jax.ShapeDtypeStruct((32, 2, 128, 128), BF)),
        in_specs=[smem, smem, vmem, vmem, vmem, vmem],
        out_specs=(vmem, vmem),
        scratch_shapes=[
            pltpu.SMEM((64,), jnp.int32), pltpu.SMEM((72,), jnp.int32),
            pltpu.VMEM((32, 128, 128), F32), pltpu.VMEM((32, 128, 128), F32),
            pltpu.VMEM((512, 128), BF), pltpu.VMEM((128, 512), BF),
            pltpu.VMEM((512, 128), BF), pltpu.VMEM((128, 512), BF),
            pltpu.VMEM((8, 128), F32), pltpu.VMEM((8, 128), F32), pltpu.VMEM((8, 128), F32),
            pltpu.VMEM((128, 512), F32),
        ],
        cost_estimate=pl.CostEstimate(flops=20_000_000_000, bytes_accessed=8_000_000, transcendentals=8_000_000),
        name="attention",
    )(order, mask, q2, do2, delta2, kvg)


OUT_LINKS = 64
LW = 448


def finish_kernel(order_ref, owner_ref, dkv, dq, x_ref, gain_ref, vis_ref, pgain_ref, wg, w2, proj,
                  tok_ref, enc_ref, w, pj, ring, stage, ysend, yrecv, hg, ng, x8, nsend, nrecv, half_out, half_in,
                  send, recv, loc):
    p = Place()
    links = Links(send, recv)
    partner = p.dev(c=1 - p.c)
    ypeer = p.dev(h=1 - p.h)
    zs = {1: p.dev(dz=1), -1: p.dev(dz=-1)}
    fan = [p.dev(dx=1), p.dev(dx=-1), p.dev(l=1 - p.l)]
    shift = [0, 3, 1, 2]
    rows = lambda dz, n: pl.ds(pl.multiple_of((((p.z + dz + 8) % 8) * 4 + (p.unit + shift[n]) % 4) * WR, 16), WR)
    held = []
    for level in (1, 0, 2):
        for n in range(4):
            held.append(pltpu.make_async_copy(wg.at[level, n], w.at[rows(level - 1, n)], loc.at[len(held)]))
    for i, dz in enumerate((-2, 2)):
        held.append(pltpu.make_async_copy(w2.at[i], w.at[rows(dz, 0)], loc.at[len(held)]))
    for cp in held:
        cp.start()
    pcopy = pltpu.make_async_copy(proj, pj, loc.at[20])
    pcopy.start()
    greet([partner, ypeer, zs[1], zs[-1]] + fan)

    sent = []
    hop = {}
    chip = lambda dz, e: pl.ds(2 * p.chip(dz, 1 - p.h if e == 0 else p.h), 2)
    nt = (((1,), (1,)), ((), ()))

    def pass_on(step, dr, e):
        dest = dr * (5 - step)
        if (step - 1, dr, e) in hop:
            hop[step - 1, dr, e].wait_recv()
            stage[step - 2, (1 - dr) // 2, e] = (
                dkv[chip(dest, e)].astype(F32) + ring[step - 2, (1 - dr) // 2, e].astype(F32)).astype(BF)
            src = stage.at[step - 2, (1 - dr) // 2, e]
        else:
            src = dkv.at[chip(dest, e)]
        hop[step, dr, e] = cp = links.copy(src, ring.at[step - 1, (1 - dr) // 2, e], zs[dr])
        cp.start()
        sent.append(cp)

    wcopies = {}

    def w_send(step, dr):
        if step == 3:
            src, dst = w2.at[(1 - dr) // 2], w.at[rows(-dr * 2, 0)]
        else:
            base = (((p.z - dr * 3 + 16) % 8) * 4 + p.unit) * WR
            src = dst = w.at[pl.ds(pl.multiple_of(base, 16), 64)] if dr == 1 else w.at[pl.ds(pl.multiple_of(base + 64, 16), 48)]
        wcopies[step, dr] = cp = links.copy(src, dst, zs[dr])
        cp.start()
        sent.append(cp)

    def spread(dz, src=None):
        part = w.at[rows(dz, 0)]
        for n, dev in enumerate(fan):
            wcopies[dz, "fan", n] = cp = links.copy(part if src is None else src, part, dev)
            cp.start()
            sent.append(cp)

    def arrived(dz):
        for n in range(3):
            wcopies[dz, "fan", n].wait_recv()

    def multiply(dz):
        level = (p.z + dz + 8) % 8
        part = w[pl.ds(pl.multiple_of(level * LW, 16), LW), 0:GW]
        ng[level] = lax.dot_general(hg[:, 0:GW], part, nt, preferred_element_type=F32)

    pass_on(1, 1, 0)
    pass_on(1, -1, 1)
    pass_on(2, 1, 1)
    pass_on(2, -1, 0)
    for dr in (1, -1):
        w_send(3, dr)
        spread(-2 * dr, w2.at[(1 - dr) // 2])
    for d in range(2):
        hg[d * 128:(d + 1) * 128, 0:GW] = dq[d]
    ready = iter(range(3))

    def near(dz):
        i = next(ready)
        for cp in held[4 * i:4 * i + 4]:
            cp.wait()
        multiply(dz)

    near(0)
    pass_on(2, 1, 0)
    pass_on(2, -1, 1)
    near(-1)
    for dr in (1, -1):
        wcopies[3, dr].wait_recv()
        w_send(4, dr)
        spread(-3 * dr)
    for dr in (1, -1):
        pass_on(3, dr, 0)
    near(1)
    for dr in (1, -1):
        pass_on(3, dr, 1)
    for cp in held[12:]:
        cp.wait()
    for dr in (1, -1):
        wcopies[4, dr].wait_recv()
    spread(4)
    for dr in (1, -1):
        pass_on(4, dr, 0)
    for dr in (1, -1):
        arrived(-2 * dr)
        multiply(-2 * dr)
    for dr in (1, -1):
        pass_on(4, dr, 1)
    square = jnp.zeros((128, 1), F32)
    for i in range(8):
        xi = x_ref[:, i * LW:(i + 1) * LW]
        x8[i] = xi
        xf = xi.astype(F32)
        square = square + jnp.sum(xf * xf, axis=1, keepdims=True)
    inverse = lax.rsqrt(square * (1.0 / D) + EPSILON)
    for dr in (1, -1):
        hop[4, dr, 0].wait_recv()
    ysend[...] = (dkv[chip(0, 0)].astype(F32) + ring[3, 0, 0].astype(F32) + ring[3, 1, 0].astype(F32)).astype(BF)
    ycopy = links.copy(ysend, yrecv, ypeer)
    ycopy.start()
    sent.append(ycopy)
    for dr in (1, -1):
        arrived(-3 * dr)
        multiply(-3 * dr)
    for dr in (1, -1):
        hop[4, dr, 1].wait_recv()
    arrived(4)
    multiply(4)
    ycopy.wait_recv()
    total = (dkv[chip(0, 1)].astype(F32) + ring[3, 0, 1].astype(F32) + ring[3, 1, 1].astype(F32) + yrecv[...].astype(F32)).astype(BF)
    for d in range(2):
        hg[d * 128:(d + 1) * 128, GW:GW + HD] = total[d, 0]
        hg[d * 128:(d + 1) * 128, GW + HD:CW] = total[d, 1]
    theirs = pl.ds(pl.multiple_of((1 - p.c) * 128, 128), 128)
    ours = pl.ds(pl.multiple_of(p.c * 128, 128), 128)
    swaps = []
    for i in range(8):
        ng[i] += lax.dot_general(hg[:, GW:CW], w[i * LW:(i + 1) * LW, GW:CW], nt, preferred_element_type=F32)
        nsend[i] = ng[i, theirs, :].astype(BF)
        cp = links.copy(nsend.at[i], nrecv.at[i], partner)
        cp.start()
        swaps.append(cp)
        sent.append(cp)
    weighted_sum = jnp.zeros((128, 1), F32)
    for i in range(8):
        swaps[i].wait_recv()
        low = (ng[i, ours, :] + nrecv[i].astype(F32)).astype(BF)
        u = low.astype(F32) * gain_ref[i * LW:(i + 1) * LW].reshape(1, LW)
        ng[i, 0:128, :] = u
        weighted_sum = weighted_sum + jnp.sum(u * x8[i].astype(F32), axis=1, keepdims=True)
    slope = inverse * inverse * inverse * (weighted_sum * (1.0 / D))
    for i in range(8):
        tok_ref[:, i * LW:(i + 1) * LW] = (inverse * ng[i, 0:128, :] - x8[i].astype(F32) * slope).astype(BF)

    first_block = order_ref[2 * p.s]
    second_block = order_ref[2 * p.s + 1]
    frame = jnp.int32(0)
    for f in range(32):
        frame = frame + jnp.where(owner_ref[f] == p.s, f, 0)
    keep_first = first_block // 2 == frame
    kept_block = jnp.where(keep_first, first_block, second_block)
    leading = kept_block % 2 == 0
    half_out[...] = jnp.where(keep_first, tok_ref[64:, :], tok_ref[:64, :])
    hcopy = links.copy(half_out, half_in, partner)
    hcopy.start()
    sent.append(hcopy)
    kept = jnp.where(keep_first, tok_ref[:64, :], tok_ref[64:, :])
    vis = vis_ref[...].astype(F32)
    centered = vis - jnp.mean(vis, axis=1, keepdims=True)
    deviation = lax.rsqrt(jnp.mean(centered * centered, axis=1, keepdims=True) + EPSILON)
    normed = centered * deviation
    pcopy.wait()
    hcopy.wait_recv()
    got = half_in[...]
    framed = jnp.concatenate([jnp.where(leading, kept, got), jnp.where(leading, got, kept)], axis=0)
    post = lax.dot_general(framed, pj[...], nt, preferred_element_type=F32)
    weighted = post * pgain_ref[...].reshape(1, CW)
    enc_ref[...] = (deviation * (
        weighted - jnp.mean(weighted, axis=1, keepdims=True)
        - normed * jnp.mean(weighted * normed, axis=1, keepdims=True))).astype(BF)
    for cp in sent:
        cp.wait_send()


def finish(order, owner, dkv, dq, x, gain, vis, pgain, wg, w2, proj):
    smem = pl.BlockSpec(memory_space=pltpu.SMEM)
    vmem = pl.BlockSpec(memory_space=pltpu.VMEM)
    hbm = pl.BlockSpec(memory_space=pl.ANY)
    block = (2, 2, 128, HD)
    return pl.pallas_call(
        finish_kernel,
        out_shape=(jax.ShapeDtypeStruct((128, D), BF), jax.ShapeDtypeStruct((128, CW), BF)),
        in_specs=[smem, smem] + [vmem] * 6 + [hbm] * 3,
        out_specs=(vmem, vmem),
        scratch_shapes=[
            pltpu.VMEM((D, CW), BF), pltpu.VMEM((CW, D), BF),
            pltpu.VMEM((4, 2, 2) + block, BF), pltpu.VMEM((3, 2, 2) + block, BF),
            pltpu.VMEM(block, BF), pltpu.VMEM(block, BF),
            pltpu.VMEM((256, CW), BF), pltpu.VMEM((8, 256, LW), F32), pltpu.VMEM((8, 128, LW), BF),
            pltpu.VMEM((8, 128, LW), BF), pltpu.VMEM((8, 128, LW), BF),
            pltpu.VMEM((64, D), BF), pltpu.VMEM((64, D), BF),
            pltpu.SemaphoreType.DMA((OUT_LINKS,)), pltpu.SemaphoreType.DMA((OUT_LINKS,)),
            pltpu.SemaphoreType.DMA((21,)),
        ],
        compiler_params=pltpu.CompilerParams(collective_id=1, has_side_effects=True),
        name="finish",
    )(order, owner, dkv, dq, x, gain, vis, pgain, wg, w2, proj)


def body(queries, keys, values, out_grad, row_delta, layer_input, norm_gain, qkv_weight,
         block_order, block_mask, frame_owner, vision_features, post_gain, projector):
    delta = jnp.pad(jnp.transpose(row_delta).reshape(2, HG, 128), ((0, 0), (0, 1), (0, 0)))
    kvg, q2, do2, delta2, wg, w2 = gather(keys, values, queries, out_grad, delta, qkv_weight)
    dq, dkv = attn(block_order, block_mask, q2, do2, delta2, kvg)
    token_grad, encoder_grad = finish(block_order, frame_owner, dkv, dq, layer_input, norm_gain, vision_features[0],
                                      post_gain, wg, w2, projector)
    return token_grad, encoder_grad[None]


def solution(mesh):
    rows = P(("batch", "seq"), None)
    cube = P(("batch", "seq"), None, None)
    placed = (rows, rows, rows, rows, rows, rows, P(), P("seq", None), P("batch"), P("batch", None), P("batch"),
              cube, P(), P())
    return jax.shard_map(body, mesh=mesh, in_specs=placed, out_specs=(rows, cube), check_vma=False)
```

```python
import jax
import jax.numpy as jnp
from jax import lax
from jax.experimental import pallas as pl
from jax.experimental.pallas import tpu as pltpu
from jax.sharding import PartitionSpec as P

HG = 7
HD = 128
GW = 896
CW = 1152
D = 3584
WR = 112
EPSILON = 1e-06
LOG2E = 1.4426950408889634
SCALE = 128 ** -0.5
TILE = 256
BF = jnp.bfloat16
F32 = jnp.float32
MESH = pl.DeviceIdType.MESH


class Place:
    def __init__(self):
        s = lax.axis_index("seq")
        b = lax.axis_index("batch")
        self.s = s
        self.c = s % 2
        self.h = (s // 2) % 2
        self.z = s // 4
        self.l = b % 2
        self.x = b // 2
        self.unit = (self.x + 2 * self.l) % 4

    def dev(self, dz=0, h=None, c=None, dx=0, l=None):
        z = (self.z + dz + 8) % 8
        x = (self.x + dx + 4) % 4
        h = self.h if h is None else h
        c = self.c if c is None else c
        l = self.l if l is None else l
        return {"seq": (z * 2 + h) * 2 + c, "batch": x * 2 + l}

    def chip(self, dz, h):
        return ((self.z + dz + 8) % 8) * 2 + h


class Links:
    def __init__(self, send, recv):
        self.send, self.recv, self.used = send, recv, 0

    def copy(self, src, dst, dev):
        i = self.used
        self.used += 1
        return pltpu.make_async_remote_copy(
            src_ref=src, dst_ref=dst, send_sem=self.send.at[i], recv_sem=self.recv.at[i],
            device_id=dev, device_id_type=MESH)


def greet(devs):
    barrier = pltpu.get_barrier_semaphore()
    for d in devs:
        pl.semaphore_signal(barrier, inc=1, device_id=d, device_id_type=MESH)
    pl.semaphore_wait(barrier, len(devs))


def weight_parts(half):
    return ((half * GW, GW, 0), (HG * 2 * HD + half * HD, HD, GW), (HG * 2 * HD + 2 * HD + half * HD, HD, GW + HD))


IN_LINKS = 96
LEVELS = 5


def gather_kernel(k_ref, v_ref, q_ref, do_ref, dl_ref, w_ref, kvg, q2, do2, dl2, wg, w2, away, wu, w0, send, recv, loc):
    p = Place()
    links = Links(send, recv)
    partner = p.dev(c=1 - p.c)
    across = [p.dev(h=1 - p.h, l=1 - p.l, c=0), p.dev(h=1 - p.h, l=1 - p.l, c=1)]
    ypeer = p.dev(h=1 - p.h)
    zs = {1: p.dev(dz=1), -1: p.dev(dz=-1)}
    fan = [p.dev(dx=1), p.dev(dx=-1), p.dev(l=1 - p.l)]
    mine, other = p.c, 1 - p.c
    col = lambda i, w: pl.ds(pl.multiple_of(i * w, 128), w)
    sent = []
    own = [pltpu.make_async_copy(k_ref.at[:, col(mine, HD)], kvg.at[p.s, 0], loc.at[0]),
           pltpu.make_async_copy(v_ref.at[:, col(mine, HD)], kvg.at[p.s, 1], loc.at[1])]
    pack = [pltpu.make_async_copy(k_ref.at[:, col(other, HD)], away.at[0], loc.at[2]),
            pltpu.make_async_copy(v_ref.at[:, col(other, HD)], away.at[1], loc.at[3])]
    rest = [pltpu.make_async_copy(q_ref.at[:, col(mine, GW)], q2.at[p.c], loc.at[4]),
            pltpu.make_async_copy(do_ref.at[:, col(mine, GW)], do2.at[p.c], loc.at[5]),
            pltpu.make_async_copy(dl_ref.at[mine], dl2.at[p.c], loc.at[6])]
    for cp in own + pack + rest:
        cp.start()
    greet([partner, ypeer] + across + [zs[1], zs[-1]] + fan)

    def begin(cp):
        cp.start()
        sent.append(cp)
        return cp

    swap = links.copy(away, kvg.at[p.s], partner)
    for cp in pack:
        cp.wait()
    begin(swap)
    for cp in own:
        cp.wait()
    kv = {}
    slot = lambda dz, e, q: 2 * p.chip(dz, p.h if e == 0 else 1 - p.h) + (p.c if q == 0 else 1 - p.c)

    def kv_send(step, e, q, dr):
        block = kvg.at[slot(-dr * (step - 1), e, q)]
        kv[step, e, q, dr] = begin(links.copy(block, block, zs[dr]))

    def y_send(q):
        block = kvg.at[slot(0, 0, q)]
        return begin(links.copy(block, block, ypeer))

    sy = {0: y_send(0)}
    for dr in (1, -1):
        kv_send(1, 0, 0, dr)

    lead = p.unit % 2 == p.c
    to_partner, to_self, to_across = [], [], []
    for i, (start, width, at) in enumerate(weight_parts(other)):
        to_partner.append(links.copy(w_ref.at[:, pl.ds(pl.multiple_of(start, 128), width)],
                                     w0.at[2 * p.h + p.c, :, pl.ds(at, width)], partner))
    for i, (start, width, at) in enumerate(weight_parts(mine)):
        to_self.append(pltpu.make_async_copy(w_ref.at[:, pl.ds(pl.multiple_of(start, 128), width)],
                                             w0.at[2 * p.h + p.c, :, pl.ds(at, width)], loc.at[7 + i]))
    for half in (0, 1):
        for i, (start, width, at) in enumerate(weight_parts(half)):
            n = links.used
            links.used += 1
            to_across.append((p.c, half, i, w_ref.at[:, pl.ds(start, width)], w0.at[2 * p.h + p.c, :, pl.ds(at, width)], n))
    first = IN_LINKS - 6
    to_across = [pltpu.make_async_remote_copy(
        src_ref=src, dst_ref=dst, send_sem=send.at[n], recv_sem=recv.at[first + 3 * d + i],
        device_id=across[half], device_id_type=MESH) for d, half, i, src, dst, n in to_across]
    from_across = [[pltpu.make_async_remote_copy(
        src_ref=w_ref.at[:, pl.ds(start, width)], dst_ref=w0.at[2 * (1 - p.h) + d, :, pl.ds(at, width)],
        send_sem=send.at[0], recv_sem=recv.at[first + 3 * d + i],
        device_id=across[0], device_id_type=MESH) for i, (start, width, at) in enumerate(weight_parts(0))] for d in (0, 1)]
    for cp in to_self:
        cp.start()
    for cp in to_partner:
        begin(cp)

    @pl.when(lead)
    def _():
        for cp in to_across:
            cp.start()

    swap.wait_recv()
    sy[1] = y_send(1)
    for dr in (1, -1):
        kv_send(1, 0, 1, dr)

    side = [links.copy(q_ref.at[:, col(other, GW)], q2.at[p.c], partner),
            links.copy(do_ref.at[:, col(other, GW)], do2.at[p.c], partner),
            links.copy(dl_ref.at[other], dl2.at[p.c], partner)]
    for cp in side:
        begin(cp)
    for q in (0, 1):
        sy[q].wait_recv()
        for dr in (1, -1):
            kv_send(1, 1, q, dr)

    wz, fans, keep = {}, {}, []

    def store(src, dst):
        cp = pltpu.make_async_copy(src, dst, loc.at[10 + len(keep)])
        cp.start()
        keep.append(cp)

    def w_send(step):
        for dr in (1, -1):
            src = w0.at[p.unit] if step == 1 else wu.at[2 - dr * (step - 1)]
            wz[step, dr] = begin(links.copy(src, wu.at[2 - dr * step], zs[dr]))

    def w_take(step):
        for dr in (1, -1):
            wz[step, dr].wait_recv()
        if step == 1:
            w_send(2)
            for dr in (1, -1):
                for n, dev in enumerate(fan):
                    fans[dr, n] = begin(links.copy(wu.at[2 - dr], wg.at[1 - dr, 1 + n], dev))
                store(wu.at[2 - dr], wg.at[1 - dr, 0])
        else:
            for dr in (1, -1):
                store(wu.at[2 - 2 * dr], w2.at[(1 - dr) // 2])

    def kv_step(step, e):
        for q in (0, 1):
            for dr in (1, -1):
                kv[step, e, q, dr].wait_recv()
                if step < 3 or (dr == 1) == (e == 0):
                    kv_send(step + 1, e, q, dr)

    for cp in to_self:
        cp.wait()
    for cp in to_partner:
        cp.wait_recv()

    for d in (0, 1):
        @pl.when(p.unit % 2 == d)
        def _():
            for cp in from_across[d]:
                cp.wait_recv()
    w_send(1)
    kv_step(1, 0)

    @pl.when(jnp.logical_not(lead))
    def _():
        for cp in to_across:
            cp.start()
    kv_step(1, 1)
    w_take(1)
    kv_step(2, 0)
    kv_step(2, 1)
    kv_step(3, 0)
    w_take(2)
    kv_step(3, 1)
    for d in (0, 1):
        @pl.when(p.unit % 2 != d)
        def _():
            for cp in from_across[d]:
                cp.wait_recv()
    for n, turn in enumerate((0, 3, 1, 2)):
        store(w0.at[(p.unit + turn) % 4], wg.at[1, n])
    for q in (0, 1):
        kv[4, 0, q, 1].wait_recv()
        kv[4, 1, q, -1].wait_recv()
    for cp in fans.values():
        cp.wait_recv()
    for cp in rest + keep:
        cp.wait()
    for cp in side:
        cp.wait_recv()
    for cp in sent:
        cp.wait_send()

    for cp in to_across:
        cp.wait_send()


def gather(keys, values, queries, out_grad, delta, weight):
    hbm = pl.BlockSpec(memory_space=pl.ANY)
    vmem = pl.BlockSpec(memory_space=pltpu.VMEM)
    return pl.pallas_call(
        gather_kernel,
        out_shape=(jax.ShapeDtypeStruct((32, 2, 128, HD), BF), jax.ShapeDtypeStruct((2, 128, GW), BF),
                   jax.ShapeDtypeStruct((2, 128, GW), BF), jax.ShapeDtypeStruct((2, 8, 128), F32),
                   jax.ShapeDtypeStruct((3, 4, WR, CW), BF), jax.ShapeDtypeStruct((2, WR, CW), BF)),
        in_specs=[hbm] * 6,
        out_specs=(vmem, vmem, vmem, vmem, hbm, hbm),
        scratch_shapes=[pltpu.VMEM((2, 128, HD), BF), pltpu.VMEM((LEVELS, WR, CW), BF), pltpu.VMEM((4, WR, CW), BF),
                        pltpu.SemaphoreType.DMA((IN_LINKS,)), pltpu.SemaphoreType.DMA((IN_LINKS,)),
                        pltpu.SemaphoreType.DMA((24,))],
        compiler_params=pltpu.CompilerParams(collective_id=0, has_side_effects=True),
        name="gather",
    )(keys, values, queries, out_grad, delta, weight)


def attn_kernel(order_ref, mask_ref, q_ref, do_ref, delta_ref, kv_ref, dq_ref, dkv_ref,
                inv_ref, live_ref, dks, dvs, qs, qt, dos, dot_, m_ref, l_ref, dl_ref, dqt):
    chip = lax.axis_index("seq") // 2

    def invert(i, _):
        inv_ref[order_ref[i]] = i
        return 0
    lax.fori_loop(0, 64, invert, 0, unroll=8)
    dks[...] = jnp.zeros_like(dks)
    dvs[...] = jnp.zeros_like(dvs)
    qs[HG * 64:, :] = jnp.zeros((64, HD), BF)
    dos[HG * 64:, :] = jnp.zeros((64, HD), BF)
    lane8 = lax.broadcasted_iota(jnp.int32, (1, 128), 1)
    ahead = lax.broadcasted_iota(jnp.int32, (64, 128), 0) - lax.broadcasted_iota(jnp.int32, (64, 128), 1) % 64

    def query_block(i, _):
        block = order_ref[4 * chip + i]
        dev, odd = i // 2, i % 2
        half = pl.multiple_of(odd * 64, 64)
        for src, st, tr in ((q_ref, qs, qt), (do_ref, dos, dot_)):
            for h in range(HG):
                st[h * 64:(h + 1) * 64, :] = src[dev, pl.ds(half, 64), h * HD:(h + 1) * HD]
            for r in range(4):
                tr[:, r * 128:(r + 1) * 128] = st[r * 128:(r + 1) * 128, :].T
        delta = delta_ref[dev]
        turned = pltpu.roll(delta, 64, 1)
        first = jnp.where(odd == 0, delta, turned)
        second = jnp.where(odd == 0, turned, delta)
        for r in range(4):
            dl_ref[r:r + 1, :] = jnp.where(lane8 < 64, first[2 * r:2 * r + 1], second[2 * r + 1:2 * r + 2])
        m_ref[...] = jnp.full_like(m_ref, -1e20)
        l_ref[...] = jnp.zeros_like(l_ref)
        dqt[...] = jnp.zeros_like(dqt)

        def collect(g, n):
            for e in range(8):
                kb = g * 8 + e
                live_ref[n] = inv_ref[kb]
                n = n + jnp.where((mask_ref[block, kb] > 0) & (kb < block), 1, 0)
            return n
        count = lax.fori_loop(0, (block + 7) // 8, collect, jnp.int32(0))
        for e in range(4):
            live_ref[count + e] = inv_ref[block]
        last = count // 4

        def places(t, n=4):
            out = []
            for e in range(n):
                k = live_ref[t * 4 + e]
                out.append((k // 2, pl.ds(pl.multiple_of((k % 2) * 64, 64), 64)))
            return out

        def bias_of(t):
            parts = []
            for e in range(4):
                index = t * 4 + e
                reach = jnp.where(index < count, 64, jnp.where(index == count, 0, -64))
                parts.append(jnp.where(ahead <= reach, 0.0, -1e30))
            return jnp.concatenate(parts, axis=0)

        def totals(t, masked, n=4):
            k = jnp.concatenate([kv_ref[d, 0, r, :] for d, r in places(t, n)], axis=0)
            s = jnp.dot(k, qt[...], preferred_element_type=F32)
            bias = bias_of(t) if masked else None
            for r in range(4):
                sh = s[:, r * 128:(r + 1) * 128] * (SCALE * LOG2E)
                if masked:
                    sh = sh + bias
                m_old = m_ref[r:r + 1, :]
                m_new = jnp.maximum(m_old, jnp.max(sh, axis=0, keepdims=True))
                p = jnp.exp2(sh - m_new)
                l_ref[r:r + 1, :] = l_ref[r:r + 1, :] * jnp.exp2(m_old - m_new) + jnp.sum(p, axis=0, keepdims=True)
                m_ref[r:r + 1, :] = m_new

        def totals_step(t, _):
            totals(2 * t, False, 8)
            return 0
        lax.fori_loop(0, last // 2, totals_step, 0)

        @pl.when(last % 2 == 1)
        def _():
            totals(last - 1, False)
        totals(last, True)
        m_ref[0:4, :] = m_ref[0:4, :] + jnp.log2(l_ref[0:4, :])

        def grads(t, masked, n=4):
            at = places(t, n)
            k = jnp.concatenate([kv_ref[d, 0, r, :] for d, r in at], axis=0)
            v = jnp.concatenate([kv_ref[d, 1, r, :] for d, r in at], axis=0)
            s = jnp.dot(k, qt[...], preferred_element_type=F32)
            dp = jnp.dot(v, dot_[...], preferred_element_type=F32)
            bias = bias_of(t) if masked else None
            ps, dss = [], []
            for r in range(4):
                cols = slice(r * 128, (r + 1) * 128)
                sh = s[:, cols] * (SCALE * LOG2E) - m_ref[r:r + 1, :]
                if masked:
                    sh = sh + bias
                p = jnp.exp2(sh)
                ds = p * (dp[:, cols] - dl_ref[r:r + 1, :])
                ps.append(p.astype(BF))
                dss.append(ds.astype(BF))
            p = jnp.concatenate(ps, axis=1)
            ds = jnp.concatenate(dss, axis=1)
            dv = jnp.dot(p, dos[...], preferred_element_type=F32)
            dk = jnp.dot(ds, qs[...], preferred_element_type=F32)
            for e, (d, r) in enumerate(at):
                dvs[d, r, :] += dv[e * 64:(e + 1) * 64]
                dks[d, r, :] += dk[e * 64:(e + 1) * 64]
            dqt[...] += jnp.dot(k.T, ds, preferred_element_type=F32)

        def grads_step(t, _):
            grads(2 * t, False, 8)
            return 0
        lax.fori_loop(0, last // 2, grads_step, 0)

        @pl.when(last % 2 == 1)
        def _():
            grads(last - 1, False)
        grads(last, True)
        for r in range(4):
            out = (dqt[:, r * 128:(r + 1) * 128].T * SCALE).astype(BF)
            for e in range(2):
                if 2 * r + e < HG:
                    dq_ref[dev, pl.ds(half, 64), (2 * r + e) * HD:(2 * r + e + 1) * HD] = out[e * 64:(e + 1) * 64]
        return 0
    lax.fori_loop(0, 4, query_block, 0)

    def write_out(d, _):
        dkv_ref[d, 0] = (dks[d] * SCALE).astype(BF)
        dkv_ref[d, 1] = dvs[d].astype(BF)
        return 0
    lax.fori_loop(0, 32, write_out, 0)


def attn(order, mask, q2, do2, delta2, kvg):
    smem = pl.BlockSpec(memory_space=pltpu.SMEM)
    vmem = pl.BlockSpec(memory_space=pltpu.VMEM)
    return pl.pallas_call(
        attn_kernel,
        out_shape=(jax.ShapeDtypeStruct((2, 128, GW), BF), jax.ShapeDtypeStruct((32, 2, 128, 128), BF)),
        in_specs=[smem, smem, vmem, vmem, vmem, vmem],
        out_specs=(vmem, vmem),
        scratch_shapes=[
            pltpu.SMEM((64,), jnp.int32), pltpu.SMEM((72,), jnp.int32),
            pltpu.VMEM((32, 128, 128), F32), pltpu.VMEM((32, 128, 128), F32),
            pltpu.VMEM((512, 128), BF), pltpu.VMEM((128, 512), BF),
            pltpu.VMEM((512, 128), BF), pltpu.VMEM((128, 512), BF),
            pltpu.VMEM((8, 128), F32), pltpu.VMEM((8, 128), F32), pltpu.VMEM((8, 128), F32),
            pltpu.VMEM((128, 512), F32),
        ],
        cost_estimate=pl.CostEstimate(flops=20_000_000_000, bytes_accessed=8_000_000, transcendentals=8_000_000),
        name="attention",
    )(order, mask, q2, do2, delta2, kvg)


OUT_LINKS = 64
LW = 448


def finish_kernel(order_ref, owner_ref, dkv, dq, x_ref, gain_ref, vis_ref, pgain_ref, wg, w2, proj,
                  tok_ref, enc_ref, w, pj, ring, stage, ysend, yrecv, hg, ng, x8, nsend, nrecv, half_out, half_in,
                  send, recv, loc):
    p = Place()
    links = Links(send, recv)
    partner = p.dev(c=1 - p.c)
    ypeer = p.dev(h=1 - p.h)
    zs = {1: p.dev(dz=1), -1: p.dev(dz=-1)}
    fan = [p.dev(dx=1), p.dev(dx=-1), p.dev(l=1 - p.l), p.dev(h=1 - p.h, l=1 - p.l)]
    shift = [0, 3, 1, 2]
    rows = lambda dz, n: pl.ds(pl.multiple_of((((p.z + dz + 8) % 8) * 4 + (p.unit + shift[n]) % 4) * WR, 16), WR)
    held = []
    for level in (1, 0, 2):
        for n in range(4):
            held.append(pltpu.make_async_copy(wg.at[level, n], w.at[rows(level - 1, n)], loc.at[len(held)]))
    for i, dz in enumerate((-2, 2)):
        held.append(pltpu.make_async_copy(w2.at[i], w.at[rows(dz, 0)], loc.at[len(held)]))
    for cp in held:
        cp.start()
    pcopy = pltpu.make_async_copy(proj, pj, loc.at[20])
    pcopy.start()
    greet([partner, ypeer, zs[1], zs[-1]] + fan)

    sent = []
    hop = {}
    chip = lambda dz, e: pl.ds(2 * p.chip(dz, 1 - p.h if e == 0 else p.h), 2)
    nt = (((1,), (1,)), ((), ()))

    def pass_on(step, dr, e):
        dest = dr * (5 - step)
        if (step - 1, dr, e) in hop:
            hop[step - 1, dr, e].wait_recv()
            stage[step - 2, (1 - dr) // 2, e] = (
                dkv[chip(dest, e)].astype(F32) + ring[step - 2, (1 - dr) // 2, e].astype(F32)).astype(BF)
            src = stage.at[step - 2, (1 - dr) // 2, e]
        else:
            src = dkv.at[chip(dest, e)]
        hop[step, dr, e] = cp = links.copy(src, ring.at[step - 1, (1 - dr) // 2, e], zs[dr])
        cp.start()
        sent.append(cp)

    wcopies = {}

    def w_send(step, dr):
        if step == 3:
            src, dst = w2.at[(1 - dr) // 2], w.at[rows(-dr * 2, 0)]
        else:
            base = (((p.z - dr * 3 + 16) % 8) * 4 + p.unit) * WR
            src = dst = w.at[pl.ds(pl.multiple_of(base, 16), 64)] if dr == 1 else w.at[pl.ds(pl.multiple_of(base + 64, 16), 48)]
        wcopies[step, dr] = cp = links.copy(src, dst, zs[dr])
        cp.start()
        sent.append(cp)

    def spread(dz, src=None):
        level = ((p.z + dz + 8) % 8) * 4 + p.unit
        for n, dev in enumerate(fan):
            first, count = ((0, WR), (0, WR), (0, 64), (64, 48))[n]
            part = w.at[pl.ds(pl.multiple_of(level * WR + first, 16), count)]
            wcopies[dz, "fan", n] = cp = links.copy(part if src is None else src.at[pl.ds(first, count)], part, dev)
            cp.start()
            sent.append(cp)

    def arrived(dz):
        for n in range(4):
            wcopies[dz, "fan", n].wait_recv()

    def multiply(dz):
        level = (p.z + dz + 8) % 8
        part = w[pl.ds(pl.multiple_of(level * LW, 16), LW), 0:GW]
        ng[level] = lax.dot_general(hg[:, 0:GW], part, nt, preferred_element_type=F32)

    pass_on(1, 1, 0)
    pass_on(1, -1, 1)
    pass_on(2, 1, 1)
    pass_on(2, -1, 0)
    for dr in (1, -1):
        w_send(3, dr)
        spread(-2 * dr, w2.at[(1 - dr) // 2])
    for d in range(2):
        hg[d * 128:(d + 1) * 128, 0:GW] = dq[d]
    ready = iter(range(3))

    def near(dz):
        i = next(ready)
        for cp in held[4 * i:4 * i + 4]:
            cp.wait()
        multiply(dz)

    near(0)
    pass_on(2, 1, 0)
    pass_on(2, -1, 1)
    near(-1)
    for dr in (1, -1):
        wcopies[3, dr].wait_recv()
        w_send(4, dr)
        spread(-3 * dr)
    for dr in (1, -1):
        pass_on(3, dr, 0)
    near(1)
    for dr in (1, -1):
        pass_on(3, dr, 1)
    for cp in held[12:]:
        cp.wait()
    for dr in (1, -1):
        wcopies[4, dr].wait_recv()
    spread(4)
    for dr in (1, -1):
        pass_on(4, dr, 0)
    for dr in (1, -1):
        arrived(-2 * dr)
        multiply(-2 * dr)
    for dr in (1, -1):
        pass_on(4, dr, 1)
    square = jnp.zeros((128, 1), F32)
    for i in range(8):
        xi = x_ref[:, i * LW:(i + 1) * LW]
        x8[i] = xi
        xf = xi.astype(F32)
        square = square + jnp.sum(xf * xf, axis=1, keepdims=True)
    inverse = lax.rsqrt(square * (1.0 / D) + EPSILON)
    for dr in (1, -1):
        hop[4, dr, 0].wait_recv()
    ysend[...] = (dkv[chip(0, 0)].astype(F32) + ring[3, 0, 0].astype(F32) + ring[3, 1, 0].astype(F32)).astype(BF)
    ycopy = links.copy(ysend, yrecv, ypeer)
    ycopy.start()
    sent.append(ycopy)
    for dr in (1, -1):
        arrived(-3 * dr)
        multiply(-3 * dr)
    for dr in (1, -1):
        hop[4, dr, 1].wait_recv()
    arrived(4)
    multiply(4)
    ycopy.wait_recv()
    total = (dkv[chip(0, 1)].astype(F32) + ring[3, 0, 1].astype(F32) + ring[3, 1, 1].astype(F32) + yrecv[...].astype(F32)).astype(BF)
    for d in range(2):
        hg[d * 128:(d + 1) * 128, GW:GW + HD] = total[d, 0]
        hg[d * 128:(d + 1) * 128, GW + HD:CW] = total[d, 1]
    theirs = pl.ds(pl.multiple_of((1 - p.c) * 128, 128), 128)
    ours = pl.ds(pl.multiple_of(p.c * 128, 128), 128)
    swaps = []
    for i in range(8):
        ng[i] += lax.dot_general(hg[:, GW:CW], w[i * LW:(i + 1) * LW, GW:CW], nt, preferred_element_type=F32)
        nsend[i] = ng[i, theirs, :].astype(BF)
        cp = links.copy(nsend.at[i], nrecv.at[i], partner)
        cp.start()
        swaps.append(cp)
        sent.append(cp)
    weighted_sum = jnp.zeros((128, 1), F32)
    for i in range(8):
        swaps[i].wait_recv()
        low = (ng[i, ours, :] + nrecv[i].astype(F32)).astype(BF)
        u = low.astype(F32) * gain_ref[i * LW:(i + 1) * LW].reshape(1, LW)
        ng[i, 0:128, :] = u
        weighted_sum = weighted_sum + jnp.sum(u * x8[i].astype(F32), axis=1, keepdims=True)
    slope = inverse * inverse * inverse * (weighted_sum * (1.0 / D))
    for i in range(8):
        tok_ref[:, i * LW:(i + 1) * LW] = (inverse * ng[i, 0:128, :] - x8[i].astype(F32) * slope).astype(BF)

    first_block = order_ref[2 * p.s]
    second_block = order_ref[2 * p.s + 1]
    frame = jnp.int32(0)
    for f in range(32):
        frame = frame + jnp.where(owner_ref[f] == p.s, f, 0)
    keep_first = first_block // 2 == frame
    kept_block = jnp.where(keep_first, first_block, second_block)
    leading = kept_block % 2 == 0
    half_out[...] = jnp.where(keep_first, tok_ref[64:, :], tok_ref[:64, :])
    hcopy = links.copy(half_out, half_in, partner)
    hcopy.start()
    sent.append(hcopy)
    kept = jnp.where(keep_first, tok_ref[:64, :], tok_ref[64:, :])
    vis = vis_ref[...].astype(F32)
    centered = vis - jnp.mean(vis, axis=1, keepdims=True)
    deviation = lax.rsqrt(jnp.mean(centered * centered, axis=1, keepdims=True) + EPSILON)
    normed = centered * deviation
    pcopy.wait()
    hcopy.wait_recv()
    got = half_in[...]
    framed = jnp.concatenate([jnp.where(leading, kept, got), jnp.where(leading, got, kept)], axis=0)
    post = lax.dot_general(framed, pj[...], nt, preferred_element_type=F32)
    weighted = post * pgain_ref[...].reshape(1, CW)
    enc_ref[...] = (deviation * (
        weighted - jnp.mean(weighted, axis=1, keepdims=True)
        - normed * jnp.mean(weighted * normed, axis=1, keepdims=True))).astype(BF)
    for cp in sent:
        cp.wait_send()


def finish(order, owner, dkv, dq, x, gain, vis, pgain, wg, w2, proj):
    smem = pl.BlockSpec(memory_space=pltpu.SMEM)
    vmem = pl.BlockSpec(memory_space=pltpu.VMEM)
    hbm = pl.BlockSpec(memory_space=pl.ANY)
    block = (2, 2, 128, HD)
    return pl.pallas_call(
        finish_kernel,
        out_shape=(jax.ShapeDtypeStruct((128, D), BF), jax.ShapeDtypeStruct((128, CW), BF)),
        in_specs=[smem, smem] + [vmem] * 6 + [hbm] * 3,
        out_specs=(vmem, vmem),
        scratch_shapes=[
            pltpu.VMEM((D, CW), BF), pltpu.VMEM((CW, D), BF),
            pltpu.VMEM((4, 2, 2) + block, BF), pltpu.VMEM((3, 2, 2) + block, BF),
            pltpu.VMEM(block, BF), pltpu.VMEM(block, BF),
            pltpu.VMEM((256, CW), BF), pltpu.VMEM((8, 256, LW), F32), pltpu.VMEM((8, 128, LW), BF),
            pltpu.VMEM((8, 128, LW), BF), pltpu.VMEM((8, 128, LW), BF),
            pltpu.VMEM((64, D), BF), pltpu.VMEM((64, D), BF),
            pltpu.SemaphoreType.DMA((OUT_LINKS,)), pltpu.SemaphoreType.DMA((OUT_LINKS,)),
            pltpu.SemaphoreType.DMA((21,)),
        ],
        compiler_params=pltpu.CompilerParams(collective_id=1, has_side_effects=True),
        name="finish",
    )(order, owner, dkv, dq, x, gain, vis, pgain, wg, w2, proj)


def body(queries, keys, values, out_grad, row_delta, layer_input, norm_gain, qkv_weight,
         block_order, block_mask, frame_owner, vision_features, post_gain, projector):
    delta = jnp.pad(jnp.transpose(row_delta).reshape(2, HG, 128), ((0, 0), (0, 1), (0, 0)))
    kvg, q2, do2, delta2, wg, w2 = gather(keys, values, queries, out_grad, delta, qkv_weight)
    dq, dkv = attn(block_order, block_mask, q2, do2, delta2, kvg)
    token_grad, encoder_grad = finish(block_order, frame_owner, dkv, dq, layer_input, norm_gain, vision_features[0],
                                      post_gain, wg, w2, projector)
    return token_grad, encoder_grad[None]


def solution(mesh):
    rows = P(("batch", "seq"), None)
    cube = P(("batch", "seq"), None, None)
    placed = (rows, rows, rows, rows, rows, rows, P(), P("seq", None), P("batch"), P("batch", None), P("batch"),
              cube, P(), P())
    return jax.shard_map(body, mesh=mesh, in_specs=placed, out_specs=(rows, cube), check_vma=False)
```

```python
import jax
import jax.numpy as jnp
from jax import lax
from jax.experimental import pallas as pl
from jax.experimental.pallas import tpu as pltpu
from jax.sharding import PartitionSpec as P

HG = 7
HD = 128
GW = 896
CW = 1152
D = 3584
WR = 112
EPSILON = 1e-06
LOG2E = 1.4426950408889634
SCALE = 128 ** -0.5
TILE = 256
BF = jnp.bfloat16
F32 = jnp.float32
MESH = pl.DeviceIdType.MESH


class Place:
    def __init__(self):
        s = lax.axis_index("seq")
        b = lax.axis_index("batch")
        self.s = s
        self.c = s % 2
        self.h = (s // 2) % 2
        self.z = s // 4
        self.l = b % 2
        self.x = b // 2
        self.unit = (self.x + 2 * self.l) % 4

    def dev(self, dz=0, h=None, c=None, dx=0, l=None):
        z = (self.z + dz + 8) % 8
        x = (self.x + dx + 4) % 4
        h = self.h if h is None else h
        c = self.c if c is None else c
        l = self.l if l is None else l
        return {"seq": (z * 2 + h) * 2 + c, "batch": x * 2 + l}

    def chip(self, dz, h):
        return ((self.z + dz + 8) % 8) * 2 + h


class Links:
    def __init__(self, send, recv):
        self.send, self.recv, self.used = send, recv, 0

    def copy(self, src, dst, dev):
        i = self.used
        self.used += 1
        return pltpu.make_async_remote_copy(
            src_ref=src, dst_ref=dst, send_sem=self.send.at[i], recv_sem=self.recv.at[i],
            device_id=dev, device_id_type=MESH)


def greet(devs):
    barrier = pltpu.get_barrier_semaphore()
    for d in devs:
        pl.semaphore_signal(barrier, inc=1, device_id=d, device_id_type=MESH)
    pl.semaphore_wait(barrier, len(devs))


def weight_parts(half):
    return ((half * GW, GW, 0), (HG * 2 * HD + half * HD, HD, GW), (HG * 2 * HD + 2 * HD + half * HD, HD, GW + HD))


IN_LINKS = 96
LEVELS = 5


def gather_kernel(k_ref, v_ref, q_ref, do_ref, dl_ref, w_ref, kvg, q2, do2, dl2, wg, w2, away, wu, w0, send, recv, loc):
    p = Place()
    links = Links(send, recv)
    partner = p.dev(c=1 - p.c)
    across = [p.dev(h=1 - p.h, l=1 - p.l, c=0), p.dev(h=1 - p.h, l=1 - p.l, c=1)]
    ypeer = p.dev(h=1 - p.h)
    zs = {1: p.dev(dz=1), -1: p.dev(dz=-1)}
    fan = [p.dev(dx=1), p.dev(dx=-1), p.dev(l=1 - p.l)]
    mine, other = p.c, 1 - p.c
    col = lambda i, w: pl.ds(pl.multiple_of(i * w, 128), w)
    sent = []
    own = [pltpu.make_async_copy(k_ref.at[:, col(mine, HD)], kvg.at[p.s, 0], loc.at[0]),
           pltpu.make_async_copy(v_ref.at[:, col(mine, HD)], kvg.at[p.s, 1], loc.at[1])]
    pack = [pltpu.make_async_copy(k_ref.at[:, col(other, HD)], away.at[0], loc.at[2]),
            pltpu.make_async_copy(v_ref.at[:, col(other, HD)], away.at[1], loc.at[3])]
    rest = [pltpu.make_async_copy(q_ref.at[:, col(mine, GW)], q2.at[p.c], loc.at[4]),
            pltpu.make_async_copy(do_ref.at[:, col(mine, GW)], do2.at[p.c], loc.at[5]),
            pltpu.make_async_copy(dl_ref.at[mine], dl2.at[p.c], loc.at[6])]
    for cp in own + pack + rest:
        cp.start()
    greet([partner, ypeer] + across + [zs[1], zs[-1]] + fan)

    def begin(cp):
        cp.start()
        sent.append(cp)
        return cp

    swap = links.copy(away, kvg.at[p.s], partner)
    for cp in pack:
        cp.wait()
    begin(swap)
    for cp in own:
        cp.wait()
    kv = {}
    slot = lambda dz, e, q: 2 * p.chip(dz, p.h if e == 0 else 1 - p.h) + (p.c if q == 0 else 1 - p.c)

    def kv_send(step, e, q, dr):
        block = kvg.at[slot(-dr * (step - 1), e, q)]
        kv[step, e, q, dr] = begin(links.copy(block, block, zs[dr]))

    def y_send(q):
        block = kvg.at[slot(0, 0, q)]
        return begin(links.copy(block, block, ypeer))

    sy = {0: y_send(0)}
    for dr in (1, -1):
        kv_send(1, 0, 0, dr)

    lead = p.unit % 2 == p.c
    to_partner, to_self, to_across = [], [], []
    for i, (start, width, at) in enumerate(weight_parts(other)):
        to_partner.append(links.copy(w_ref.at[:, pl.ds(pl.multiple_of(start, 128), width)],
                                     w0.at[2 * p.h + p.c, :, pl.ds(at, width)], partner))
    for i, (start, width, at) in enumerate(weight_parts(mine)):
        to_self.append(pltpu.make_async_copy(w_ref.at[:, pl.ds(pl.multiple_of(start, 128), width)],
                                             w0.at[2 * p.h + p.c, :, pl.ds(at, width)], loc.at[7 + i]))
    for half in (0, 1):
        for i, (start, width, at) in enumerate(weight_parts(half)):
            n = links.used
            links.used += 1
            to_across.append((p.c, half, i, w_ref.at[:, pl.ds(start, width)], w0.at[2 * p.h + p.c, :, pl.ds(at, width)], n))
    first = IN_LINKS - 6
    to_across = [pltpu.make_async_remote_copy(
        src_ref=src, dst_ref=dst, send_sem=send.at[n], recv_sem=recv.at[first + 3 * d + i],
        device_id=across[half], device_id_type=MESH) for d, half, i, src, dst, n in to_across]
    from_across = [[pltpu.make_async_remote_copy(
        src_ref=w_ref.at[:, pl.ds(start, width)], dst_ref=w0.at[2 * (1 - p.h) + d, :, pl.ds(at, width)],
        send_sem=send.at[0], recv_sem=recv.at[first + 3 * d + i],
        device_id=across[0], device_id_type=MESH) for i, (start, width, at) in enumerate(weight_parts(0))] for d in (0, 1)]
    for cp in to_self:
        cp.start()
    for cp in to_partner:
        begin(cp)

    @pl.when(lead)
    def _():
        for cp in to_across:
            cp.start()

    swap.wait_recv()
    sy[1] = y_send(1)
    for dr in (1, -1):
        kv_send(1, 0, 1, dr)

    side = [links.copy(q_ref.at[:, col(other, GW)], q2.at[p.c], partner),
            links.copy(do_ref.at[:, col(other, GW)], do2.at[p.c], partner),
            links.copy(dl_ref.at[other], dl2.at[p.c], partner)]
    for cp in side:
        begin(cp)
    for q in (0, 1):
        sy[q].wait_recv()
        for dr in (1, -1):
            kv_send(1, 1, q, dr)

    wz, fans, keep = {}, {}, []

    def store(src, dst):
        cp = pltpu.make_async_copy(src, dst, loc.at[10 + len(keep)])
        cp.start()
        keep.append(cp)

    def w_send(step):
        for dr in (1, -1):
            src = w0.at[p.unit] if step == 1 else wu.at[2 - dr * (step - 1)]
            wz[step, dr] = begin(links.copy(src, wu.at[2 - dr * step], zs[dr]))

    def w_take(step):
        for dr in (1, -1):
            wz[step, dr].wait_recv()
        if step == 1:
            w_send(2)
            for dr in (1, -1):
                for n, dev in enumerate(fan):
                    fans[dr, n] = begin(links.copy(wu.at[2 - dr], wg.at[1 - dr, 1 + n], dev))
                store(wu.at[2 - dr], wg.at[1 - dr, 0])
        else:
            for dr in (1, -1):
                store(wu.at[2 - 2 * dr], w2.at[(1 - dr) // 2])

    def kv_step(step, e):
        for q in (0, 1):
            for dr in (1, -1):
                kv[step, e, q, dr].wait_recv()
                if step < 3 or (dr == 1) == (e == 0):
                    kv_send(step + 1, e, q, dr)

    for cp in to_self:
        cp.wait()
    for cp in to_partner:
        cp.wait_recv()

    for d in (0, 1):
        @pl.when(p.unit % 2 == d)
        def _():
            for cp in from_across[d]:
                cp.wait_recv()
    w_send(1)
    kv_step(1, 0)

    @pl.when(jnp.logical_not(lead))
    def _():
        for cp in to_across:
            cp.start()
    kv_step(1, 1)
    w_take(1)
    kv_step(2, 0)
    kv_step(2, 1)
    kv_step(3, 0)
    w_take(2)
    kv_step(3, 1)
    for d in (0, 1):
        @pl.when(p.unit % 2 != d)
        def _():
            for cp in from_across[d]:
                cp.wait_recv()
    for n, turn in enumerate((0, 3, 1, 2)):
        store(w0.at[(p.unit + turn) % 4], wg.at[1, n])
    for q in (0, 1):
        kv[4, 0, q, 1].wait_recv()
        kv[4, 1, q, -1].wait_recv()
    for cp in fans.values():
        cp.wait_recv()
    for cp in rest + keep:
        cp.wait()
    for cp in side:
        cp.wait_recv()
    for cp in sent:
        cp.wait_send()

    for cp in to_across:
        cp.wait_send()


def gather(keys, values, queries, out_grad, delta, weight):
    hbm = pl.BlockSpec(memory_space=pl.ANY)
    vmem = pl.BlockSpec(memory_space=pltpu.VMEM)
    return pl.pallas_call(
        gather_kernel,
        out_shape=(jax.ShapeDtypeStruct((32, 2, 128, HD), BF), jax.ShapeDtypeStruct((2, 128, GW), BF),
                   jax.ShapeDtypeStruct((2, 128, GW), BF), jax.ShapeDtypeStruct((2, 8, 128), F32),
                   jax.ShapeDtypeStruct((3, 4, WR, CW), BF), jax.ShapeDtypeStruct((2, WR, CW), BF)),
        in_specs=[hbm] * 6,
        out_specs=(vmem, vmem, vmem, vmem, hbm, hbm),
        scratch_shapes=[pltpu.VMEM((2, 128, HD), BF), pltpu.VMEM((LEVELS, WR, CW), BF), pltpu.VMEM((4, WR, CW), BF),
                        pltpu.SemaphoreType.DMA((IN_LINKS,)), pltpu.SemaphoreType.DMA((IN_LINKS,)),
                        pltpu.SemaphoreType.DMA((24,))],
        compiler_params=pltpu.CompilerParams(collective_id=0, has_side_effects=True),
        name="gather",
    )(keys, values, queries, out_grad, delta, weight)


def attn_kernel(order_ref, mask_ref, q_ref, do_ref, delta_ref, kv_ref, dq_ref, dkv_ref,
                inv_ref, live_ref, dks, dvs, qs, qt, dos, dot_, m_ref, l_ref, dl_ref, dqt):
    chip = lax.axis_index("seq") // 2

    def invert(i, _):
        inv_ref[order_ref[i]] = i
        return 0
    lax.fori_loop(0, 64, invert, 0, unroll=8)
    dks[...] = jnp.zeros_like(dks)
    dvs[...] = jnp.zeros_like(dvs)
    qs[HG * 64:, :] = jnp.zeros((64, HD), BF)
    dos[HG * 64:, :] = jnp.zeros((64, HD), BF)
    lane8 = lax.broadcasted_iota(jnp.int32, (1, 128), 1)
    ahead = lax.broadcasted_iota(jnp.int32, (64, 128), 0) - lax.broadcasted_iota(jnp.int32, (64, 128), 1) % 64

    def query_block(i, _):
        block = order_ref[4 * chip + i]
        dev, odd = i // 2, i % 2
        half = pl.multiple_of(odd * 64, 64)
        for src, st, tr in ((q_ref, qs, qt), (do_ref, dos, dot_)):
            for h in range(HG):
                st[h * 64:(h + 1) * 64, :] = src[dev, pl.ds(half, 64), h * HD:(h + 1) * HD]
            for r in range(4):
                tr[:, r * 128:(r + 1) * 128] = st[r * 128:(r + 1) * 128, :].T
        delta = delta_ref[dev]
        turned = pltpu.roll(delta, 64, 1)
        first = jnp.where(odd == 0, delta, turned)
        second = jnp.where(odd == 0, turned, delta)
        for r in range(4):
            dl_ref[r:r + 1, :] = jnp.where(lane8 < 64, first[2 * r:2 * r + 1], second[2 * r + 1:2 * r + 2])
        m_ref[...] = jnp.full_like(m_ref, -1e20)
        l_ref[...] = jnp.zeros_like(l_ref)
        dqt[...] = jnp.zeros_like(dqt)

        def collect(g, n):
            for e in range(8):
                kb = g * 8 + e
                live_ref[n] = inv_ref[kb]
                n = n + jnp.where((mask_ref[block, kb] > 0) & (kb < block), 1, 0)
            return n
        count = lax.fori_loop(0, (block + 7) // 8, collect, jnp.int32(0))
        for e in range(4):
            live_ref[count + e] = inv_ref[block]
        last = count // 4

        def places(t, n=4):
            out = []
            for e in range(n):
                k = live_ref[t * 4 + e]
                out.append((k // 2, pl.ds(pl.multiple_of((k % 2) * 64, 64), 64)))
            return out

        def bias_of(t):
            parts = []
            for e in range(4):
                index = t * 4 + e
                reach = jnp.where(index < count, 64, jnp.where(index == count, 0, -64))
                parts.append(jnp.where(ahead <= reach, 0.0, -1e30))
            return jnp.concatenate(parts, axis=0)

        def totals(t, masked, n=4):
            k = jnp.concatenate([kv_ref[d, 0, r, :] for d, r in places(t, n)], axis=0)
            s = jnp.dot(k, qt[...], preferred_element_type=F32)
            bias = bias_of(t) if masked else None
            for r in range(4):
                sh = s[:, r * 128:(r + 1) * 128] * (SCALE * LOG2E)
                if masked:
                    sh = sh + bias
                m_old = m_ref[r:r + 1, :]
                m_new = jnp.maximum(m_old, jnp.max(sh, axis=0, keepdims=True))
                p = jnp.exp2(sh - m_new)
                l_ref[r:r + 1, :] = l_ref[r:r + 1, :] * jnp.exp2(m_old - m_new) + jnp.sum(p, axis=0, keepdims=True)
                m_ref[r:r + 1, :] = m_new

        def totals_step(t, _):
            totals(2 * t, False, 8)
            return 0
        lax.fori_loop(0, last // 2, totals_step, 0)

        @pl.when(last % 2 == 1)
        def _():
            totals(last - 1, False)
        totals(last, True)
        m_ref[0:4, :] = m_ref[0:4, :] + jnp.log2(l_ref[0:4, :])

        def grads(t, masked, n=4):
            at = places(t, n)
            k = jnp.concatenate([kv_ref[d, 0, r, :] for d, r in at], axis=0)
            v = jnp.concatenate([kv_ref[d, 1, r, :] for d, r in at], axis=0)
            s = jnp.dot(k, qt[...], preferred_element_type=F32)
            dp = jnp.dot(v, dot_[...], preferred_element_type=F32)
            bias = bias_of(t) if masked else None
            ps, dss = [], []
            for r in range(4):
                cols = slice(r * 128, (r + 1) * 128)
                sh = s[:, cols] * (SCALE * LOG2E) - m_ref[r:r + 1, :]
                if masked:
                    sh = sh + bias
                p = jnp.exp2(sh)
                ds = p * (dp[:, cols] - dl_ref[r:r + 1, :])
                ps.append(p.astype(BF))
                dss.append(ds.astype(BF))
            p = jnp.concatenate(ps, axis=1)
            ds = jnp.concatenate(dss, axis=1)
            dv = jnp.dot(p, dos[...], preferred_element_type=F32)
            dk = jnp.dot(ds, qs[...], preferred_element_type=F32)
            for e, (d, r) in enumerate(at):
                dvs[d, r, :] += dv[e * 64:(e + 1) * 64]
                dks[d, r, :] += dk[e * 64:(e + 1) * 64]
            dqt[...] += jnp.dot(k.T, ds, preferred_element_type=F32)

        def grads_step(t, _):
            grads(2 * t, False, 8)
            return 0
        lax.fori_loop(0, last // 2, grads_step, 0)

        @pl.when(last % 2 == 1)
        def _():
            grads(last - 1, False)
        grads(last, True)
        for r in range(4):
            out = (dqt[:, r * 128:(r + 1) * 128].T * SCALE).astype(BF)
            for e in range(2):
                if 2 * r + e < HG:
                    dq_ref[dev, pl.ds(half, 64), (2 * r + e) * HD:(2 * r + e + 1) * HD] = out[e * 64:(e + 1) * 64]
        return 0
    lax.fori_loop(0, 4, query_block, 0)

    def write_out(d, _):
        dkv_ref[d, 0] = (dks[d] * SCALE).astype(BF)
        dkv_ref[d, 1] = dvs[d].astype(BF)
        return 0
    lax.fori_loop(0, 32, write_out, 0)


def attn(order, mask, q2, do2, delta2, kvg):
    smem = pl.BlockSpec(memory_space=pltpu.SMEM)
    vmem = pl.BlockSpec(memory_space=pltpu.VMEM)
    return pl.pallas_call(
        attn_kernel,
        out_shape=(jax.ShapeDtypeStruct((2, 128, GW), BF), jax.ShapeDtypeStruct((32, 2, 128, 128), BF)),
        in_specs=[smem, smem, vmem, vmem, vmem, vmem],
        out_specs=(vmem, vmem),
        scratch_shapes=[
            pltpu.SMEM((64,), jnp.int32), pltpu.SMEM((72,), jnp.int32),
            pltpu.VMEM((32, 128, 128), F32), pltpu.VMEM((32, 128, 128), F32),
            pltpu.VMEM((512, 128), BF), pltpu.VMEM((128, 512), BF),
            pltpu.VMEM((512, 128), BF), pltpu.VMEM((128, 512), BF),
            pltpu.VMEM((8, 128), F32), pltpu.VMEM((8, 128), F32), pltpu.VMEM((8, 128), F32),
            pltpu.VMEM((128, 512), F32),
        ],
        cost_estimate=pl.CostEstimate(flops=20_000_000_000, bytes_accessed=8_000_000, transcendentals=8_000_000),
        name="attention",
    )(order, mask, q2, do2, delta2, kvg)


OUT_LINKS = 64
LW = 448


def finish_kernel(order_ref, owner_ref, dkv, dq, x_ref, gain_ref, vis_ref, pgain_ref, wg, w2, proj,
                  tok_ref, enc_ref, w, pj, ring, stage, ysend, yrecv, hg, ng, x8, nsend, nrecv, half_out, half_in,
                  send, recv, loc):
    p = Place()
    links = Links(send, recv)
    partner = p.dev(c=1 - p.c)
    ypeer = p.dev(h=1 - p.h)
    zs = {1: p.dev(dz=1), -1: p.dev(dz=-1)}
    fan = [p.dev(dx=1), p.dev(dx=-1), p.dev(l=1 - p.l), p.dev(h=1 - p.h, l=1 - p.l)]
    shift = [0, 3, 1, 2]
    rows = lambda dz, n: pl.ds(pl.multiple_of((((p.z + dz + 8) % 8) * 4 + (p.unit + shift[n]) % 4) * WR, 16), WR)
    held = []
    for level in (1, 0, 2):
        for n in range(4):
            held.append(pltpu.make_async_copy(wg.at[level, n], w.at[rows(level - 1, n)], loc.at[len(held)]))
    for i, dz in enumerate((-2, 2)):
        held.append(pltpu.make_async_copy(w2.at[i], w.at[rows(dz, 0)], loc.at[len(held)]))
    for cp in held:
        cp.start()
    pcopy = pltpu.make_async_copy(proj, pj, loc.at[20])
    greet([partner, ypeer, zs[1], zs[-1]] + fan)

    sent = []
    hop = {}
    chip = lambda dz, e: pl.ds(2 * p.chip(dz, 1 - p.h if e == 0 else p.h), 2)
    nt = (((1,), (1,)), ((), ()))

    def pass_on(step, dr, e):
        dest = dr * (5 - step)
        if (step - 1, dr, e) in hop:
            hop[step - 1, dr, e].wait_recv()
            stage[step - 2, (1 - dr) // 2, e] = (
                dkv[chip(dest, e)].astype(F32) + ring[step - 2, (1 - dr) // 2, e].astype(F32)).astype(BF)
            src = stage.at[step - 2, (1 - dr) // 2, e]
        else:
            src = dkv.at[chip(dest, e)]
        hop[step, dr, e] = cp = links.copy(src, ring.at[step - 1, (1 - dr) // 2, e], zs[dr])
        cp.start()
        sent.append(cp)

    wcopies = {}

    def w_send(step, dr):
        if step == 3:
            src, dst = w2.at[(1 - dr) // 2], w.at[rows(-dr * 2, 0)]
        else:
            base = (((p.z - dr * 3 + 16) % 8) * 4 + p.unit) * WR
            src = dst = w.at[pl.ds(pl.multiple_of(base, 16), 64)] if dr == 1 else w.at[pl.ds(pl.multiple_of(base + 64, 16), 48)]
        wcopies[step, dr] = cp = links.copy(src, dst, zs[dr])
        cp.start()
        sent.append(cp)

    def spread(dz, src=None):
        level = ((p.z + dz + 8) % 8) * 4 + p.unit
        for n, dev in enumerate(fan):
            first, count = ((0, WR), (0, WR), (0, 64), (64, 48))[n]
            part = w.at[pl.ds(pl.multiple_of(level * WR + first, 16), count)]
            wcopies[dz, "fan", n] = cp = links.copy(part if src is None else src.at[pl.ds(first, count)], part, dev)
            cp.start()
            sent.append(cp)

    def arrived(dz):
        for n in range(4):
            wcopies[dz, "fan", n].wait_recv()

    def multiply(dz):
        level = (p.z + dz + 8) % 8
        part = w[pl.ds(pl.multiple_of(level * LW, 16), LW), 0:GW]
        ng[level] = lax.dot_general(hg[:, 0:GW], part, nt, preferred_element_type=F32)

    pass_on(1, 1, 0)
    pass_on(1, -1, 1)
    pass_on(2, 1, 1)
    pass_on(2, -1, 0)
    for dr in (1, -1):
        w_send(3, dr)
        spread(-2 * dr, w2.at[(1 - dr) // 2])
    for d in range(2):
        hg[d * 128:(d + 1) * 128, 0:GW] = dq[d]
    ready = iter(range(3))

    def near(dz):
        i = next(ready)
        for cp in held[4 * i:4 * i + 4]:
            cp.wait()
        multiply(dz)

    near(0)
    pcopy.start()
    pass_on(2, 1, 0)
    pass_on(2, -1, 1)
    near(-1)
    for dr in (1, -1):
        wcopies[3, dr].wait_recv()
        w_send(4, dr)
        spread(-3 * dr)
    for dr in (1, -1):
        pass_on(3, dr, 0)
    near(1)
    for dr in (1, -1):
        pass_on(3, dr, 1)
    for cp in held[12:]:
        cp.wait()
    for dr in (1, -1):
        wcopies[4, dr].wait_recv()
    spread(4)
    for dr in (1, -1):
        pass_on(4, dr, 0)
    for dr in (1, -1):
        arrived(-2 * dr)
        multiply(-2 * dr)
    for dr in (1, -1):
        pass_on(4, dr, 1)
    square = jnp.zeros((128, 1), F32)
    for i in range(8):
        xi = x_ref[:, i * LW:(i + 1) * LW]
        x8[i] = xi
        xf = xi.astype(F32)
        square = square + jnp.sum(xf * xf, axis=1, keepdims=True)
    inverse = lax.rsqrt(square * (1.0 / D) + EPSILON)
    for dr in (1, -1):
        hop[4, dr, 0].wait_recv()
    ysend[...] = (dkv[chip(0, 0)].astype(F32) + ring[3, 0, 0].astype(F32) + ring[3, 1, 0].astype(F32)).astype(BF)
    ycopy = links.copy(ysend, yrecv, ypeer)
    ycopy.start()
    sent.append(ycopy)
    for dr in (1, -1):
        arrived(-3 * dr)
        multiply(-3 * dr)
    for dr in (1, -1):
        hop[4, dr, 1].wait_recv()
    arrived(4)
    multiply(4)
    ycopy.wait_recv()
    total = (dkv[chip(0, 1)].astype(F32) + ring[3, 0, 1].astype(F32) + ring[3, 1, 1].astype(F32) + yrecv[...].astype(F32)).astype(BF)
    for d in range(2):
        hg[d * 128:(d + 1) * 128, GW:GW + HD] = total[d, 0]
        hg[d * 128:(d + 1) * 128, GW + HD:CW] = total[d, 1]
    theirs = pl.ds(pl.multiple_of((1 - p.c) * 128, 128), 128)
    ours = pl.ds(pl.multiple_of(p.c * 128, 128), 128)
    swaps = []
    for i in range(8):
        ng[i] += lax.dot_general(hg[:, GW:CW], w[i * LW:(i + 1) * LW, GW:CW], nt, preferred_element_type=F32)
        nsend[i] = ng[i, theirs, :].astype(BF)
        cp = links.copy(nsend.at[i], nrecv.at[i], partner)
        cp.start()
        swaps.append(cp)
        sent.append(cp)
    weighted_sum = jnp.zeros((128, 1), F32)
    for i in range(8):
        swaps[i].wait_recv()
        low = (ng[i, ours, :] + nrecv[i].astype(F32)).astype(BF)
        u = low.astype(F32) * gain_ref[i * LW:(i + 1) * LW].reshape(1, LW)
        ng[i, 0:128, :] = u
        weighted_sum = weighted_sum + jnp.sum(u * x8[i].astype(F32), axis=1, keepdims=True)
    slope = inverse * inverse * inverse * (weighted_sum * (1.0 / D))
    for i in range(8):
        tok_ref[:, i * LW:(i + 1) * LW] = (inverse * ng[i, 0:128, :] - x8[i].astype(F32) * slope).astype(BF)

    first_block = order_ref[2 * p.s]
    second_block = order_ref[2 * p.s + 1]
    frame = jnp.int32(0)
    for f in range(32):
        frame = frame + jnp.where(owner_ref[f] == p.s, f, 0)
    keep_first = first_block // 2 == frame
    kept_block = jnp.where(keep_first, first_block, second_block)
    leading = kept_block % 2 == 0
    half_out[...] = jnp.where(keep_first, tok_ref[64:, :], tok_ref[:64, :])
    hcopy = links.copy(half_out, half_in, partner)
    hcopy.start()
    sent.append(hcopy)
    kept = jnp.where(keep_first, tok_ref[:64, :], tok_ref[64:, :])
    vis = vis_ref[...].astype(F32)
    centered = vis - jnp.mean(vis, axis=1, keepdims=True)
    deviation = lax.rsqrt(jnp.mean(centered * centered, axis=1, keepdims=True) + EPSILON)
    normed = centered * deviation
    pcopy.wait()
    hcopy.wait_recv()
    got = half_in[...]
    framed = jnp.concatenate([jnp.where(leading, kept, got), jnp.where(leading, got, kept)], axis=0)
    post = lax.dot_general(framed, pj[...], nt, preferred_element_type=F32)
    weighted = post * pgain_ref[...].reshape(1, CW)
    enc_ref[...] = (deviation * (
        weighted - jnp.mean(weighted, axis=1, keepdims=True)
        - normed * jnp.mean(weighted * normed, axis=1, keepdims=True))).astype(BF)
    for cp in sent:
        cp.wait_send()


def finish(order, owner, dkv, dq, x, gain, vis, pgain, wg, w2, proj):
    smem = pl.BlockSpec(memory_space=pltpu.SMEM)
    vmem = pl.BlockSpec(memory_space=pltpu.VMEM)
    hbm = pl.BlockSpec(memory_space=pl.ANY)
    block = (2, 2, 128, HD)
    return pl.pallas_call(
        finish_kernel,
        out_shape=(jax.ShapeDtypeStruct((128, D), BF), jax.ShapeDtypeStruct((128, CW), BF)),
        in_specs=[smem, smem] + [vmem] * 6 + [hbm] * 3,
        out_specs=(vmem, vmem),
        scratch_shapes=[
            pltpu.VMEM((D, CW), BF), pltpu.VMEM((CW, D), BF),
            pltpu.VMEM((4, 2, 2) + block, BF), pltpu.VMEM((3, 2, 2) + block, BF),
            pltpu.VMEM(block, BF), pltpu.VMEM(block, BF),
            pltpu.VMEM((256, CW), BF), pltpu.VMEM((8, 256, LW), F32), pltpu.VMEM((8, 128, LW), BF),
            pltpu.VMEM((8, 128, LW), BF), pltpu.VMEM((8, 128, LW), BF),
            pltpu.VMEM((64, D), BF), pltpu.VMEM((64, D), BF),
            pltpu.SemaphoreType.DMA((OUT_LINKS,)), pltpu.SemaphoreType.DMA((OUT_LINKS,)),
            pltpu.SemaphoreType.DMA((21,)),
        ],
        compiler_params=pltpu.CompilerParams(collective_id=1, has_side_effects=True),
        name="finish",
    )(order, owner, dkv, dq, x, gain, vis, pgain, wg, w2, proj)


def body(queries, keys, values, out_grad, row_delta, layer_input, norm_gain, qkv_weight,
         block_order, block_mask, frame_owner, vision_features, post_gain, projector):
    delta = jnp.pad(jnp.transpose(row_delta).reshape(2, HG, 128), ((0, 0), (0, 1), (0, 0)))
    kvg, q2, do2, delta2, wg, w2 = gather(keys, values, queries, out_grad, delta, qkv_weight)
    dq, dkv = attn(block_order, block_mask, q2, do2, delta2, kvg)
    token_grad, encoder_grad = finish(block_order, frame_owner, dkv, dq, layer_input, norm_gain, vision_features[0],
                                      post_gain, wg, w2, projector)
    return token_grad, encoder_grad[None]


def solution(mesh):
    rows = P(("batch", "seq"), None)
    cube = P(("batch", "seq"), None, None)
    placed = (rows, rows, rows, rows, rows, rows, P(), P("seq", None), P("batch"), P("batch", None), P("batch"),
              cube, P(), P())
    return jax.shard_map(body, mesh=mesh, in_specs=placed, out_specs=(rows, cube), check_vma=False)
```
